256 devices in a mesh: gx: 32 (over z_lo, y, core), gy: 8 (over z_hi, x).
Axes of the slice: x: 4, y: 4, z: 8 (z_hi: 2, z_lo: 4; z = z_hi * 4 + z_lo), core: 2. Of those that a mesh axis runs over, the one named last changes fastest.
Arguments:
- e_field: float32 [3, 64, 256, 1024], P(None, None, 'gx', 'gy'), may hold values from -6 to 6
- h_field: float32 [3, 64, 256, 1024], P(None, None, 'gx', 'gy'), may hold values from -6 to 6
- material: int32 [64, 256, 1024], P(None, 'gx', 'gy'), may hold values from 0 to 7
- permittivity: float32 [8], replicated, may hold values from 1 to 12
- conductivity: float32 [8], replicated, may hold values from 0.05 to 2
- src_shift: int32 [2048, 2], P(('gx', 'gy')), may hold values from 0 to 128
- src_weight: float32 [2048], P(('gx', 'gy')), may hold values from 0.05 to 5
- pupil_mask: int32 [128, 128], replicated, may hold values 0 or 1
Outputs:
- image: float32 [512, 512], P(('gx', 'gy'))
- e_final: float32 [3, 64, 256, 1024], P(None, None, 'gx', 'gy')
- h_final: float32 [3, 64, 256, 1024], P(None, None, 'gx', 'gy')
The draws below stay inside these ranges and needn't reach their ends.
All inputs are finite; a program needn't handle non-finite values.
Results may differ from the reference program's by a relative error of at most 0.0019.
Values may be sent and summed in bfloat16 or wider, within the bound.
No kernel may reach another device: no remote copies, remote signals or barrier semaphores. Data moves between devices by JAX's collectives and lax.ppermute only.
A program may use at most 128 MiB of HBM per device.

```python
import math
import jax
import jax.numpy as jnp
from jax import lax

NZ = 64
STEPS = 4
MATS = 8
K = 256
PW = 128
IMG = 512
NX = 256
NY = 1024
SOURCES = 2048


def with_ends(drawn, rng, low, largest):
    longest = drawn.shape.index(max(drawn.shape))
    spots = []
    for shift in (0, 1):
        where = [jax.random.randint(jax.random.fold_in(rng, axis), (), 0, length) for axis, length in enumerate(drawn.shape)]
        where[longest] = (where[longest] + shift) % drawn.shape[longest]
        spots.append(tuple(where))
    return drawn.at[spots[0]].set(low).at[spots[1]].set(largest)


def steps_of(stream_key, extent, split, least, largest):
    loudness, own = 1.0, jax.random.fold_in(stream_key, 6)
    for position, blocks in split:
        draws = jnp.exp(jax.random.uniform(jax.random.fold_in(own, position), (blocks,), jnp.float32, least / len(split), largest / len(split)))
        loudness = loudness * jnp.repeat(draws, extent[position] // blocks).reshape([-1 if axis == position else 1 for axis in range(len(extent))])
    return loudness


def scatter_about(own_key, dims, width, limit, shards=(), kind=jnp.bfloat16):
    result = width * jax.random.normal(own_key, dims, jnp.float32)
    if shards:
        result = result * steps_of(own_key, dims, shards, -0.22, 0.18)
    return jnp.clip(result, -limit, limit).astype(kind)


def setup_inputs(seed: int = 0) -> dict:
    splits = jax.random.split(jax.random.key(seed), 9)
    e_field = scatter_about(splits[0], (3, NZ, NX, NY), 1.0, 6.0, ((2, 32), (3, 8)), jnp.float32)
    h_field = scatter_about(splits[1], (3, NZ, NX, NY), 1.0, 6.0, ((2, 32), (3, 8)), jnp.float32)
    material = with_ends(jax.random.randint(splits[2], (NZ, NX, NY), 0, MATS), jax.random.fold_in(splits[2], 1), 0, MATS - 1).astype(jnp.int32)
    permittivity = jnp.clip(jnp.exp(jax.random.uniform(splits[3], (MATS,), jnp.float32, math.log(1.0), math.log(12.0))), 1.0, 12.0)
    conductivity = jnp.clip(jnp.exp(jax.random.uniform(splits[4], (MATS,), jnp.float32, math.log(0.05), math.log(2.0))), 0.05, 2.0)
    src_shift = with_ends(jax.random.randint(splits[5], (SOURCES, 2), 0, K - PW + 1), jax.random.fold_in(splits[5], 1), 0, K - PW).astype(jnp.int32)
    src_weight = jnp.clip(jnp.exp(math.log(5.0) - 4.6051702 * jax.random.uniform(splits[6], (SOURCES,), jnp.float32) ** steps_of(splits[6], (SOURCES,), ((0, 256),), -0.2, 0.2)), 0.05, 5.0)
    pupil_mask = with_ends((jax.random.randint(splits[7], (PW, PW), 0, 4) < 3).astype(jnp.int32), jax.random.fold_in(splits[7], 1), 0, 1)
    return dict(e_field=e_field, h_field=h_field, material=material, permittivity=permittivity, conductivity=conductivity, src_shift=src_shift, src_weight=src_weight, pupil_mask=pupil_mask)


COURANT = 0.5

def coefficients(material, permittivity, conductivity):
    loss = conductivity / (2.0 * permittivity)
    keep_tab = (1.0 - loss) / (1.0 + loss)
    drive_tab = COURANT / (permittivity * (1.0 + loss))
    keep = jnp.zeros(material.shape, jnp.float32)
    drive = jnp.zeros(material.shape, jnp.float32)
    for index in range(permittivity.shape[0]):
        chosen = material == index
        keep = jnp.where(chosen, keep_tab[index], keep)
        drive = jnp.where(chosen, drive_tab[index], drive)
    return (keep, drive)

def zero_face(field, axis):
    shape = list(field.shape)
    shape[axis] = 1
    return jnp.zeros(shape, field.dtype)

def ahead(field, face, axis):
    count = field.shape[axis]
    return jnp.concatenate((lax.slice_in_dim(field, 1, count, axis=axis), face), axis=axis)

def behind(field, face, axis):
    count = field.shape[axis]
    return jnp.concatenate((face, lax.slice_in_dim(field, 0, count - 1, axis=axis)), axis=axis)

def magnetic(e, h, faces_x, faces_y):
    ex, ey, ez = (e[0], e[1], e[2])
    ey_x = ahead(ey, faces_x[0], 1)
    ez_x = ahead(ez, faces_x[1], 1)
    ex_y = ahead(ex, faces_y[0], 2)
    ez_y = ahead(ez, faces_y[1], 2)
    ex_z = ahead(ex, zero_face(ex, 0), 0)
    ey_z = ahead(ey, zero_face(ey, 0), 0)
    new_x = h[0] - COURANT * (ez_y - ez - (ey_z - ey))
    new_y = h[1] - COURANT * (ex_z - ex - (ez_x - ez))
    new_z = h[2] - COURANT * (ey_x - ey - (ex_y - ex))
    return jnp.stack((new_x, new_y, new_z))

def electric(e, h, keep, drive, faces_x, faces_y):
    hx, hy, hz = (h[0], h[1], h[2])
    hy_x = behind(hy, faces_x[0], 1)
    hz_x = behind(hz, faces_x[1], 1)
    hx_y = behind(hx, faces_y[0], 2)
    hz_y = behind(hz, faces_y[1], 2)
    hx_z = behind(hx, zero_face(hx, 0), 0)
    hy_z = behind(hy, zero_face(hy, 0), 0)
    new_x = keep * e[0] + drive * (hz - hz_y - (hy - hy_z))
    new_y = keep * e[1] + drive * (hx - hx_z - (hz - hz_x))
    new_z = keep * e[2] + drive * (hy - hy_x - (hx - hx_y))
    return jnp.stack((new_x, new_y, new_z))

def exit_spectrum(near, row_start, col_start, rows_all, cols_all, order):
    count_x = near.shape[1]
    count_y = near.shape[2]
    freqs = jnp.arange(order, dtype=jnp.int32) - order // 2
    cols = col_start + jnp.arange(count_y, dtype=jnp.int32)
    phase_y = jnp.mod(cols[:, None] * freqs[None, :], cols_all).astype(jnp.float32) * (2.0 * math.pi / cols_all)
    table_y = jnp.concatenate((jnp.cos(phase_y), -jnp.sin(phase_y)), axis=1)
    half = jnp.dot(near.reshape(2 * count_x, count_y), table_y, precision=lax.Precision.HIGHEST)
    half = half.reshape(2, count_x, 2 * order)
    rows = row_start + jnp.arange(count_x, dtype=jnp.int32)
    phase_x = jnp.mod(freqs[:, None] * rows[None, :], rows_all).astype(jnp.float32) * (2.0 * math.pi / rows_all)
    table_x = jnp.concatenate((jnp.cos(phase_x), jnp.sin(phase_x)), axis=0)
    blocks = jnp.einsum('ax,pxb->pab', table_x, half, precision=lax.Precision.HIGHEST)
    real = blocks[:, :order, :order] + blocks[:, order:, order:]
    imag = blocks[:, :order, order:] - blocks[:, order:, :order]
    stacked = jnp.stack((real[0], imag[0], real[1], imag[1]), axis=1)
    return stacked * (1.0 / math.sqrt(rows_all * cols_all))

def pupil_tables(window, pixels):
    offsets = jnp.arange(window, dtype=jnp.int32) - window // 2
    places = jnp.arange(pixels, dtype=jnp.int32)
    phase = jnp.mod(offsets[:, None] * places[None, :], pixels).astype(jnp.float32) * (2.0 * math.pi / pixels)
    cosine = jnp.cos(phase)
    sine = jnp.sin(phase)
    second = jnp.concatenate((jnp.concatenate((cosine, sine), axis=1), jnp.concatenate((-sine, cosine), axis=1)), axis=0)
    row_cos = cosine.T / window
    row_sin = sine.T / window
    real_row = jnp.stack((row_cos, -row_sin), axis=2)
    imag_row = jnp.stack((row_sin, row_cos), axis=2)
    first = jnp.stack((real_row, imag_row)).reshape(2, pixels, 2 * window)
    return (second.astype(jnp.bfloat16), first.astype(jnp.bfloat16))

def pupil_halves(spectrum_b, shifts, pupil_mask, second, window, pixels):
    zero = jnp.zeros((), jnp.int32)

    def cut(shift):
        return lax.dynamic_slice(spectrum_b, (shift[0].astype(jnp.int32), zero, shift[1].astype(jnp.int32)), (window, 4, window))
    pieces = jax.vmap(cut)(shifts)
    pieces = pieces * pupil_mask.astype(jnp.bfloat16)[None, :, None, :]
    count = shifts.shape[0]
    arranged = pieces.reshape(count, window, 2, 2, window).transpose(0, 2, 1, 3, 4).reshape(count * 2 * window, 2 * window)
    halves = jnp.dot(arranged, second, preferred_element_type=jnp.float32).astype(jnp.bfloat16)
    return halves.reshape(count * 2, 2 * window, pixels)

def reference(e_field, h_field, material, permittivity, conductivity, src_shift, src_weight, pupil_mask):
    keep, drive = coefficients(material, permittivity, conductivity)
    e = e_field
    h = h_field
    for step in range(STEPS):
        faces_x = (zero_face(e[1], 1), zero_face(e[2], 1))
        faces_y = (zero_face(e[0], 2), zero_face(e[2], 2))
        h = magnetic(e, h, faces_x, faces_y)
        faces_x = (zero_face(h[1], 1), zero_face(h[2], 1))
        faces_y = (zero_face(h[0], 2), zero_face(h[2], 2))
        e = electric(e, h, keep, drive, faces_x, faces_y)
    near = e[0:2, NZ - 1]
    spectrum = exit_spectrum(near, 0, 0, NX, NY, K)
    spectrum_b = spectrum.astype(jnp.bfloat16)
    second, first = pupil_tables(PW, IMG)
    flat_first = first.reshape(2 * IMG, 2 * PW)
    total_sources = src_shift.shape[0]

    def add(image, item):
        shift, weight = item
        halves = pupil_halves(spectrum_b, shift[None, :], pupil_mask, second, PW, IMG)
        for pol in range(2):
            field = jnp.dot(flat_first, halves[pol], preferred_element_type=jnp.float32)
            image = image + weight / total_sources * (field[:IMG] * field[:IMG] + field[IMG:] * field[IMG:])
        return (image, None)
    image, _ = lax.scan(add, jnp.zeros((IMG, IMG), jnp.float32), (src_shift, src_weight))
    return (image, e, h)
```

```python
import numpy as np
import jax
import jax.numpy as jnp
from jax import lax
from jax.experimental import pallas as pl
from jax.experimental.pallas import tpu as pltpu
from jax.sharding import Mesh
from jax.sharding import PartitionSpec as P

STEPS = 4
COURANT = 0.5
NZ = 64
K = 256
PW = 128
IMG = 512
GRID = IMG // 2
MATS = 8
SOURCES = 2048
TOP = 5
BLOCK = 8
GX = ("zl", "y", "c")
GY = ("zh", "x")
ALL = GX + GY
F32 = jnp.float32
BF16 = jnp.bfloat16


def split_bf16(table):
    high = table.astype(np.float32).astype(jnp.bfloat16)
    low = (table - high.astype(np.float64)).astype(np.float32).astype(jnp.bfloat16)
    return high, low


def tables(rows_all, cols_all):
    freqs = np.arange(K) - K // 2
    phase_y = 2.0 * np.pi * (np.outer(np.arange(cols_all // 2), freqs) % cols_all) / cols_all
    ty = np.concatenate((np.cos(phase_y), -np.sin(phase_y)), axis=1)
    phase_x = 2.0 * np.pi * (np.outer(freqs, np.arange(rows_all)) % rows_all) / rows_all
    tx = np.concatenate((np.cos(phase_x), np.sin(phase_x)), axis=0)
    offsets = np.arange(PW) - PW // 2
    places = 2 * np.arange(GRID)
    phase = 2.0 * np.pi * (np.outer(offsets, places) % IMG) / IMG
    cosine, sine = np.cos(phase), np.sin(phase)
    seconds = []
    for half in range(2):
        c = cosine[:, half * 128 : half * 128 + 128]
        s = sine[:, half * 128 : half * 128 + 128]
        seconds.append(np.concatenate((np.concatenate((c, s), 1), np.concatenate((-s, c), 1)), 0))
    second = np.stack(seconds).astype(np.float32).astype(jnp.bfloat16)
    rc, rs = cosine.T / PW, sine.T / PW
    first = np.concatenate((np.concatenate((rc, -rs), 1), np.concatenate((rs, rc), 1)), 0)
    first = first.astype(np.float32).astype(jnp.bfloat16)
    lag = np.arange(-IMG, IMG + 1)
    orders = np.arange(1, GRID // 2)
    kernel = 1.0 + 2.0 * np.cos(2.0 * np.pi * np.outer(lag, orders) / IMG).sum(1)
    kernel = (kernel + np.cos(2.0 * np.pi * (GRID // 2) * lag / IMG)) / GRID
    between = np.arange(IMG)[:, None] - 2 * np.arange(GRID)[None, :]
    upsample = kernel[between + IMG]
    upsample[::2] = np.eye(GRID)
    return split_bf16(ty) + split_bf16(tx) + (second, first, upsample.astype(np.float32))


def sub_iota(shape):
    return lax.broadcasted_iota(jnp.int32, shape, len(shape) - 2)


def lane_iota(shape):
    return lax.broadcasted_iota(jnp.int32, shape, len(shape) - 1)


def pair_rows(near, far):
    turned = pltpu.roll(far, 4, axis=far.ndim - 2)
    low = sub_iota(near.shape) < 4
    return jnp.where(low, turned, near), jnp.where(low, near, turned)


def unpair_rows(up, down):
    low = sub_iota(up.shape) < 4
    near = jnp.where(low, down, up)
    far = pltpu.roll(jnp.where(low, up, down), 4, axis=up.ndim - 2)
    return near, far


def component(e_ref, h_ref, mat_ref, comp):
    if comp < 3:
        return e_ref[comp]
    if comp < 6:
        return h_ref[comp - 3]
    return (mat_ref[...] + 1).astype(F32)


def strip_kernel(e_ref, h_ref, mat_ref, shift_ref, weight_ref, low_ref, high_ref):
    slot = (lane_iota((4, 8, 128)) + 4) // 8 % 16
    first = lane_iota((2, 8, 128)) % 8 < 4
    for comp in range(7):
        layers = component(e_ref, h_ref, mat_ref, comp).reshape(4, 16, 8, 128)
        strip = layers[:, 0]
        for s in range(1, 16):
            strip = jnp.where(slot == s, pltpu.roll(layers[:, s], 8 * s, axis=2), strip)
        turned = pltpu.roll(strip[2:], 4, axis=2)
        low_ref[pl.ds(2 * comp, 2)] = jnp.where(first, strip[:2], turned)
        high_ref[pl.ds(2 * comp, 2)] = jnp.where(first, turned, strip[:2])
    row = sub_iota((8, 128))
    lane = lane_iota((8, 128))
    info = jnp.zeros((8, 128), F32)
    for s in range(8):
        here = row == s
        info = jnp.where(here & (lane == 0), shift_ref[0, s].astype(F32), info)
        info = jnp.where(here & (lane == 1), shift_ref[1, s].astype(F32), info)
        info = jnp.where(here & (lane == 2), weight_ref[s], info)
    low_ref[14] = info
    high_ref[14] = info


def rows_kernel(e_ref, h_ref, mat_ref, after_ref, up_ref, down_ref):
    for comp in range(7):
        block = component(e_ref, h_ref, mat_ref, comp)
        up, down = pair_rows(block[:32], block[32:])
        up_ref[comp] = up
        down_ref[comp] = down


def corner_kernel(low_ref, high_ref, own_ref, strip_ref, up_ref, down_ref):
    first = lane_iota((2, 8, 128)) % 8 < 4
    for comp in range(7):
        low = low_ref[pl.ds(2 * comp, 2)]
        high = high_ref[pl.ds(2 * comp, 2)]
        near = jnp.where(first, high, low)
        far = pltpu.roll(jnp.where(first, low, high), 124, axis=2)
        strip_ref[pl.ds(4 * comp, 2)] = near
        strip_ref[pl.ds(4 * comp + 2, 2)] = far
        up, down = pair_rows(near, far)
        up_ref[pl.ds(2 * comp, 2)] = up
        down_ref[pl.ds(2 * comp, 2)] = down
    odd = lax.axis_index("x") % 2 == 1
    other = jnp.where(odd, low_ref[14], high_ref[14])
    info = jnp.where(lane_iota((8, 128)) < 8, own_ref[14], pltpu.roll(other, 8, axis=1))
    strip_ref[28] = info
    up_ref[14] = info
    down_ref[14] = info


def lookup(code, eps_ref, sig_ref):
    keep = jnp.zeros(code.shape, F32)
    drive = jnp.zeros(code.shape, F32)
    one = jnp.ones((8, 128), F32)
    for index in range(MATS):
        eps = one * eps_ref[index]
        loss = (one * sig_ref[index]) / (2.0 * eps)
        keep_one = ((1.0 - loss) / (1.0 + loss))[:1, :1]
        drive_one = (COURANT / (eps * (1.0 + loss)))[:1, :1]
        chosen = code == index + 1.0
        keep = jnp.where(chosen, keep_one, keep)
        drive = jnp.where(chosen, drive_one, drive)
    return keep, drive


def wide(own, near_row, strip, corner, slot):
    turn = (128 - 8 * slot) % 128
    if turn:
        strip = pltpu.roll(strip, turn, axis=1)
        corner = pltpu.roll(corner, turn, axis=1)
    return jnp.concatenate(
        (jnp.concatenate((own, strip), axis=1), jnp.concatenate((near_row, corner), axis=1)), axis=0
    )


def ahead(field, axis):
    return pltpu.roll(field, field.shape[axis] - 1, axis=axis)


def behind(field, axis):
    return pltpu.roll(field, 1, axis=axis)


def magnetic(e, e_next, h, inside):
    ex, ey, ez = e
    new_x = h[0] - COURANT * (ahead(ez, 1) - ez - (e_next[1] - ey))
    new_y = h[1] - COURANT * (e_next[0] - ex - (ahead(ez, 0) - ez))
    new_z = h[2] - COURANT * (ahead(ey, 0) - ey - (ahead(ex, 1) - ex))
    return new_x * inside, new_y * inside, new_z * inside


def electric(e, h, h_last, keep, drive):
    hx, hy, hz = h
    new_x = keep * e[0] + drive * (hz - behind(hz, 1) - (hy - h_last[1]))
    new_y = keep * e[1] + drive * (hx - h_last[0] - (hz - behind(hz, 0)))
    new_z = keep * e[2] + drive * (hy - behind(hy, 0) - (hx - behind(hx, 1)))
    return new_x, new_y, new_z


def near_kernel(
    e_ref, h_ref, mat_ref, up_ref, down_ref, strip_ref, cup_ref, cdown_ref, eps_ref, sig_ref,
    near_ref, info_ref,
):
    fields = []
    for comp in range(7):
        _, far = unpair_rows(up_ref[comp], down_ref[comp])
        _, corner = unpair_rows(cup_ref[2 * comp + 1], cdown_ref[2 * comp + 1])
        strip = strip_ref[4 * comp + 3]
        layers = []
        for z in range(8 - TOP, 8):
            if comp < 3:
                own = e_ref[comp, z]
            elif comp < 6:
                own = h_ref[comp - 3, z]
            else:
                own = (mat_ref[z] + 1).astype(F32)
            layers.append(wide(own, far[z], strip, corner, 8 + z))
        fields.append(layers)
    e = [tuple(fields[c][z] for c in range(3)) for z in range(TOP)]
    h = [tuple(fields[c + 3][z] for c in range(3)) for z in range(TOP)]
    zero = jnp.zeros((16, 256), F32)
    coefs = []
    for z in range(TOP):
        code = fields[6][z]
        coefs.append(lookup(code, eps_ref, sig_ref) + ((code > 0.5).astype(F32),))
    for step in range(STEPS):
        for z in range(step, TOP):
            keep, drive, inside = coefs[z]
            e_next = e[z + 1] if z + 1 < TOP else (zero, zero)
            h[z] = magnetic(e[z], e_next, h[z], inside)
            if z > step:
                e[z] = electric(e[z], h[z], h[z - 1], keep, drive)
    for pol in range(2):
        tile = e[TOP - 1][pol][:8, :128].astype(BF16)
        near_ref[:, pol] = jnp.broadcast_to(tile, (16, 8, 8, 128))
    up = lax.axis_index("c") == 1
    other = jnp.where(up, cup_ref[14], cdown_ref[14])
    info_ref[...] = jnp.where(
        lane_iota((8, 128)) < 16, strip_ref[28], pltpu.roll(other, 16, axis=1)
    )


def yee_kernel(
    e_ref, h_ref, mat_ref, up_ref, down_ref, strip_ref, cup_ref, cdown_ref, eps_ref, sig_ref,
    e_out, h_out, e_s, h_s, c_s,
):
    for comp in range(3):
        e_s[comp, NZ] = jnp.zeros((16, 256), F32)
        h_s[comp, 0] = jnp.zeros((16, 256), F32)
    for comp in range(7):
        near, far = unpair_rows(up_ref[comp], down_ref[comp])
        c_near, c_far = unpair_rows(
            cup_ref[pl.ds(2 * comp, 2)], cdown_ref[pl.ds(2 * comp, 2)]
        )
        for z in range(NZ):
            group, slot = divmod(z, 16)
            rows = near[z] if z < 32 else far[z - 32]
            corner = c_near[group] if group < 2 else c_far[group - 2]
            if comp < 3:
                own = e_ref[comp, z]
            elif comp < 6:
                own = h_ref[comp - 3, z]
            else:
                own = (mat_ref[z] + 1).astype(F32)
            value = wide(own, rows, strip_ref[4 * comp + group], corner, slot)
            if comp < 3:
                e_s[comp, z] = value
            elif comp < 6:
                h_s[comp - 3, z + 1] = value
            else:
                c_s[2, z] = value

    def coef(z, carry):
        code = c_s[2, z]
        keep, drive = lookup(code, eps_ref, sig_ref)
        c_s[0, z] = keep
        c_s[1, z] = drive
        c_s[2, z] = (code > 0.5).astype(F32)
        return carry

    lax.fori_loop(0, NZ, coef, 0)

    def step(k, carry):
        def block(i, carry):
            first = i * BLOCK
            for j in range(BLOCK):
                z = first + j
                e = tuple(e_s[c, z] for c in range(3))
                e_next = (e_s[0, z + 1], e_s[1, z + 1])
                h = tuple(h_s[c, z + 1] for c in range(3))
                h = magnetic(e, e_next, h, c_s[2, z])
                for c in range(3):
                    h_s[c, z + 1] = h[c]
            for j in range(BLOCK):
                z = first + j
                e = tuple(e_s[c, z] for c in range(3))
                h = tuple(h_s[c, z + 1] for c in range(3))
                e = electric(e, h, (h_s[0, z], h_s[1, z]), c_s[0, z], c_s[1, z])
                for c in range(3):
                    e_s[c, z] = e[c]
            return carry

        return lax.fori_loop(0, NZ // BLOCK, block, carry)

    lax.fori_loop(0, STEPS, step, 0)
    for comp in range(3):
        e_out[comp] = e_s[comp, pl.ds(0, NZ), pl.ds(0, 8), pl.ds(0, 128)]
        h_out[comp] = h_s[comp, pl.ds(1, NZ), pl.ds(0, 8), pl.ds(0, 128)]


def dot(a, b):
    return jnp.dot(a, b, preferred_element_type=F32)


def cut(ref, a, b):
    turn = (128 - b) % 128
    first = pltpu.roll(ref[0, pl.ds(a, PW), :], turn, axis=1)
    second = pltpu.roll(ref[1, pl.ds(a, PW), :], turn, axis=1)
    lane = lane_iota((PW, 128))
    return jnp.where(lane + b < 128, first, second)


def image_kernel(
    place_ref, info_ref, recv_ref, tyh_ref, tyl_ref, txh_ref, txl_ref, second_ref, first_ref,
    up_ref, mask_ref, out_ref, near_s, re_s, im_s, half_s, acc_s,
):
    for j in range(8):
        tile = recv_ref[:, j].astype(F32).reshape(K, 128)
        near_s[pl.ds(K * (j // 4), K), pl.ds(128 * (j % 4), 128)] = tile.astype(BF16)
    near = near_s[...]
    both = dot(near, tyh_ref[...]) + dot(near, tyl_ref[...])
    half = both[:K] + jnp.where(lane_iota((1, 2 * K)) % 2 == 0, both[K:], -both[K:])
    half_h = half.astype(BF16)
    half_l = (half - half_h.astype(F32)).astype(BF16)
    blocks = dot(txh_ref[...], half_h) + (dot(txh_ref[...], half_l) + dot(txl_ref[...], half_h))
    scale = 1.0 / 512.0
    real = (blocks[:K, :K] + blocks[K:, K:]) * scale
    imag = (blocks[:K, K:] - blocks[K:, :K]) * scale
    real = real.astype(BF16).astype(F32)
    imag = imag.astype(BF16).astype(F32)
    for t in range(2):
        re_s[t] = real[:, 128 * t : 128 * t + 128]
        im_s[t] = imag[:, 128 * t : 128 * t + 128]
    mask = mask_ref[...].astype(F32)
    side = lax.axis_index("x") % 2

    def cuts(i, carry):
        for t in range(8):
            a = place_ref[t, 8 * i]
            b = place_ref[t, 8 * i + 1]
            window = jnp.concatenate(
                (cut(re_s, a, b) * mask, cut(im_s, a, b) * mask), axis=1
            ).astype(BF16)
            half = dot(window, second_ref[side]).astype(BF16)
            half_s[i, pl.ds(0, 128), pl.ds(128 * t, 128)] = half[:, :128]
            half_s[i, pl.ds(128, 128), pl.ds(128 * t, 128)] = half[:, 128:]
        return carry

    lax.fori_loop(0, 4, cuts, 0)
    acc_s[...] = jnp.zeros(acc_s.shape, F32)

    def fields(i, carry):
        field = dot(first_ref[...], half_s[i])
        power = field[:GRID] * field[:GRID] + field[GRID:] * field[GRID:]
        total = acc_s[...]
        for t in range(8):
            weight = info_ref[t, 8 * i + 2] * (1.0 / SOURCES)
            total = total + power[:, 128 * t : 128 * t + 128] * weight
        acc_s[...] = total
        return carry

    lax.fori_loop(0, 4, fields, 0)
    out_ref[...] = jnp.dot(
        up_ref[...], acc_s[...], precision=lax.Precision.HIGHEST, preferred_element_type=F32
    )


def sum_kernel(recv_ref, up_ref, out_ref):
    total = jnp.sum(recv_ref[...].reshape(64, 8, 128), axis=0)
    total = total + pltpu.roll(total, 4, axis=0)
    line = jnp.concatenate((total, pltpu.roll(total, 6, axis=0)), axis=1)
    full = lax.dot_general(
        line, up_ref[...], (((1,), (1,)), ((), ())), precision=lax.Precision.HIGHEST,
        preferred_element_type=F32,
    )
    out_ref[...] = full[:2]


def shifted(value, axes, by):
    count = lax.axis_size(axes)
    return lax.ppermute(value, axes, [(i, i + by) for i in range(count) if 0 <= i + by < count])


def local(
    e_field, h_field, material, permittivity, conductivity, src_shift, src_weight, pupil_mask
):
    rows_all = e_field.shape[2] * lax.axis_size(GX)
    cols_all = e_field.shape[3] * lax.axis_size(GY)
    tyh, tyl, txh, txl, second, first, upsample = tables(rows_all, cols_all)
    smem = pl.BlockSpec(memory_space=pltpu.SMEM)
    vmem = pl.BlockSpec(memory_space=pltpu.VMEM)

    def shape(*dims, dtype=F32):
        return jax.ShapeDtypeStruct(dims, dtype)

    to_low, to_high = pl.pallas_call(
        strip_kernel,
        out_shape=(shape(15, 8, 128), shape(15, 8, 128)),
        in_specs=[vmem, vmem, vmem, smem, smem],
        out_specs=(vmem, vmem),
        name="strip",
    )(e_field, h_field, material, src_shift.T, src_weight)
    low = shifted(to_high, GY, 1)
    high = shifted(to_low, GY, -1)
    up, down = pl.pallas_call(
        rows_kernel,
        out_shape=(shape(7, 32, 8, 128), shape(7, 32, 8, 128)),
        in_specs=[vmem, vmem, vmem, pl.BlockSpec(memory_space=pl.ANY)],
        out_specs=(vmem, vmem),
        name="rows",
    )(e_field, h_field, material, to_low)
    up_in = shifted(up, GX, 1)
    down_in = shifted(down, GX, -1)
    strip, cup, cdown = pl.pallas_call(
        corner_kernel,
        out_shape=(shape(29, 8, 128), shape(15, 8, 128), shape(15, 8, 128)),
        in_specs=[vmem] * 3,
        out_specs=(vmem,) * 3,
        name="corner",
    )(low, high, to_low)
    cup_in = shifted(cup, GX, 1)
    cdown_in = shifted(cdown, GX, -1)

    field = pl.BlockSpec((3, 8, 8, 128), lambda i: (0, 7, 0, 0))
    rows = pl.BlockSpec((7, 8, 8, 128), lambda i: (0, 3, 0, 0))
    near, info = pl.pallas_call(
        near_kernel,
        grid=(1,),
        out_shape=(shape(16, 2, 8, 8, 128, dtype=BF16), shape(8, 128)),
        in_specs=[
            field, field, pl.BlockSpec((8, 8, 128), lambda i: (7, 0, 0)), rows, rows,
            pl.BlockSpec((29, 8, 128), lambda i: (0, 0, 0)),
            pl.BlockSpec((15, 8, 128), lambda i: (0, 0, 0)),
            pl.BlockSpec((15, 8, 128), lambda i: (0, 0, 0)), smem, smem,
        ],
        out_specs=(
            pl.BlockSpec((16, 2, 8, 8, 128), lambda i: (0, 0, 0, 0, 0)),
            pl.BlockSpec((8, 128), lambda i: (0, 0)),
        ),
        name="near",
    )(e_field, h_field, material, up_in, down_in, strip, cup_in, cdown_in, permittivity, conductivity)
    recv = lax.all_to_all(near.reshape(256, 8, 128), ALL, 0, 0, tiled=True)

    e_final, h_final = pl.pallas_call(
        yee_kernel,
        out_shape=(shape(*e_field.shape), shape(*h_field.shape)),
        in_specs=[vmem] * 8 + [smem, smem],
        out_specs=(vmem, vmem),
        scratch_shapes=[
            pltpu.VMEM((3, NZ + 1, 16, 256), F32),
            pltpu.VMEM((3, NZ + 1, 16, 256), F32),
            pltpu.VMEM((3, NZ, 16, 256), F32),
        ],
        cost_estimate=pl.CostEstimate(flops=40000000, transcendentals=0, bytes_accessed=8000000),
        name="yee",
    )(e_field, h_field, material, up_in, down_in, strip, cup_in, cdown_in, permittivity, conductivity)

    partial = pl.pallas_call(
        image_kernel,
        out_shape=shape(2 * GRID, 128),
        in_specs=[smem, smem] + [vmem] * 9,
        out_specs=vmem,
        scratch_shapes=[
            pltpu.VMEM((2 * K, 512), BF16),
            pltpu.VMEM((2, K, 128), F32),
            pltpu.VMEM((2, K, 128), F32),
            pltpu.VMEM((4, 256, 1024), BF16),
            pltpu.VMEM((GRID, 128), F32),
        ],
        name="image",
    )(
        info.astype(jnp.int32), info, recv.reshape(32, 8, 8, 128), tyh, tyl, txh, txl, second,
        first, upsample, pupil_mask,
    )
    pieces = lax.all_to_all(partial.reshape(256, 2, 128), ALL, 0, 0, tiled=True)
    image = pl.pallas_call(
        sum_kernel,
        out_shape=shape(2, IMG),
        in_specs=[vmem, vmem],
        out_specs=vmem,
        name="total",
    )(pieces.reshape(512, 128), upsample)
    return image, e_final, h_final


def solution(mesh):
    finer = Mesh(mesh.devices.reshape(4, 4, 2, 2, 4), ALL)
    return jax.shard_map(
        local,
        mesh=finer,
        in_specs=(
            P(None, None, GX, GY),
            P(None, None, GX, GY),
            P(None, GX, GY),
            P(),
            P(),
            P(ALL, None),
            P(ALL),
            P(),
        ),
        out_specs=(P(ALL, None), P(None, None, GX, GY), P(None, None, GX, GY)),
        check_vma=False,
    )
```

```python
import numpy as np
import jax
import jax.numpy as jnp
from jax import lax
from jax.experimental import pallas as pl
from jax.experimental.pallas import tpu as pltpu
from jax.sharding import Mesh
from jax.sharding import PartitionSpec as P


STEPS = 4
COURANT = 0.5
NZ = 64
K = 256
PW = 128
IMG = 512
GRID = IMG // 2
MATS = 8
SOURCES = 2048
TOP = 5
BLOCK = 16
THIN = 36
GX = ("zl", "y", "c")
GY = ("zh", "x")
ALL = GX + GY
F32 = jnp.float32
BF16 = jnp.bfloat16


def split_bf16(table):
    high = table.astype(np.float32).astype(jnp.bfloat16)
    low = (table - high.astype(np.float64)).astype(np.float32).astype(jnp.bfloat16)
    return high, low


def tables(rows_all, cols_all):
    freqs = np.arange(K) - K // 2
    phase_y = 2.0 * np.pi * (np.outer(np.arange(cols_all // 2) + STEPS, freqs) % cols_all) / cols_all
    ty = np.concatenate((np.cos(phase_y), -np.sin(phase_y)), axis=1)
    phase_x = 2.0 * np.pi * (np.outer(freqs, np.arange(rows_all) + STEPS) % rows_all) / rows_all
    tx = np.concatenate((np.cos(phase_x), np.sin(phase_x)), axis=0)
    offsets = np.arange(PW) - PW // 2
    places = 2 * np.arange(GRID)
    phase = 2.0 * np.pi * (np.outer(offsets, places) % IMG) / IMG
    cosine, sine = np.cos(phase), np.sin(phase)
    seconds = []
    for half in range(2):
        c = cosine[:, half * 128 : half * 128 + 128]
        s = sine[:, half * 128 : half * 128 + 128]
        seconds.append(np.concatenate((np.concatenate((c, s), 1), np.concatenate((-s, c), 1)), 0))
    second = np.stack(seconds).astype(np.float32).astype(jnp.bfloat16)
    rc, rs = cosine.T / PW, sine.T / PW
    first = np.concatenate((np.concatenate((rc, -rs), 1), np.concatenate((rs, rc), 1)), 0)
    first = first.astype(np.float32).astype(jnp.bfloat16)
    lag = np.arange(-IMG, IMG + 1)
    orders = np.arange(1, GRID // 2)
    kernel = 1.0 + 2.0 * np.cos(2.0 * np.pi * np.outer(lag, orders) / IMG).sum(1)
    kernel = (kernel + np.cos(2.0 * np.pi * (GRID // 2) * lag / IMG)) / GRID
    between = np.arange(IMG)[:, None] - 2 * np.arange(GRID)[None, :]
    upsample = kernel[between + IMG]
    upsample[::2] = np.eye(GRID)
    return split_bf16(ty) + split_bf16(tx) + (second, first, upsample.astype(np.float32))


def sub_iota(shape):
    return lax.broadcasted_iota(jnp.int32, shape, len(shape) - 2)


def lane_iota(shape):
    return lax.broadcasted_iota(jnp.int32, shape, len(shape) - 1)


def pair_rows(near, far):
    turned = pltpu.roll(far, 4, axis=far.ndim - 2)
    low = sub_iota(near.shape) < 4
    return jnp.where(low, turned, near), jnp.where(low, near, turned)


def unpair_rows(up, down):
    low = sub_iota(up.shape) < 4
    near = jnp.where(low, down, up)
    far = pltpu.roll(jnp.where(low, up, down), 4, axis=up.ndim - 2)
    return near, far


def component(e_ref, h_ref, mat_ref, comp):
    if comp < 3:
        return e_ref[comp]
    if comp < 6:
        return h_ref[comp - 3]
    return (mat_ref[...] + 1).astype(F32)


def thin_component(e_ref, h_ref, mat_ref, comp, z):
    if comp < 3:
        return e_ref[comp, z]
    if comp < 6:
        return h_ref[comp - 3, z]
    return (mat_ref[z] + 1).astype(F32)


def packed_strip(block):
    slot = (lane_iota((4, 8, 128)) + 4) // 8 % 16
    layers = block.reshape(4, 16, 8, 128)
    strip = layers[:, 0]
    for s in range(1, 16):
        strip = jnp.where(slot == s, pltpu.roll(layers[:, s], 8 * s, axis=2), strip)
    return strip[:2], pltpu.roll(strip[2:], 4, axis=2)


def thin_kernel(e_ref, h_ref, mat_ref, shift_ref, weight_ref, down_ref, low_ref):
    slot = lane_iota((8, 128)) // 8
    thin = []
    for comp in range(7):
        for z in range(8 - TOP, 8):
            thin.append(thin_component(e_ref, h_ref, mat_ref, comp, z))
    for k, tile in enumerate(thin):
        down_ref[k] = tile
    for g in range(3):
        strip = thin[16 * g]
        for s, tile in enumerate(thin[16 * g + 1 : 16 * g + 16]):
            strip = jnp.where(slot == s + 1, pltpu.roll(tile, 8 * (s + 1), axis=1), strip)
        low_ref[g] = strip
    row = sub_iota((8, 128))
    lane = lane_iota((8, 128))
    info = jnp.zeros((8, 128), F32)
    for s in range(8):
        here = row == s
        info = jnp.where(here & (lane == 0), shift_ref[0, s].astype(F32), info)
        info = jnp.where(here & (lane == 1), shift_ref[1, s].astype(F32), info)
        info = jnp.where(here & (lane == 2), weight_ref[s], info)
    down_ref[THIN - 1] = info
    low_ref[3] = info


def strip_kernel(e_ref, h_ref, mat_ref, after_ref, low_ref, high_ref):
    first = lane_iota((2, 8, 128)) % 8 < 4
    for comp in range(7):
        near, far = packed_strip(component(e_ref, h_ref, mat_ref, comp))
        low_ref[pl.ds(2 * comp, 2)] = jnp.where(first, near, far)
        high_ref[pl.ds(2 * comp, 2)] = jnp.where(first, far, near)


def rows_kernel(e_ref, h_ref, mat_ref, after_ref, up_ref, down_ref):
    for comp in range(7):
        block = component(e_ref, h_ref, mat_ref, comp)
        up, down = pair_rows(block[:32], block[32:])
        up_ref[pl.ds(32 * comp, 32)] = up
        down_ref[pl.ds(32 * comp, 32)] = down


def at_end(axes, last):
    flag = None
    for axis in axes:
        here = lax.axis_index(axis) == (lax.axis_size(axis) - 1 if last else 0)
        flag = here if flag is None else flag & here
    return flag


def corner_kernel(low_ref, high_ref, strip_ref, up_ref, down_ref):
    first = lane_iota((2, 8, 128)) % 8 < 4
    no_low, no_high = at_end(GY, False), at_end(GY, True)
    for comp in range(7):
        low = jnp.where(no_low, 0.0, low_ref[pl.ds(2 * comp, 2)])
        high = jnp.where(no_high, 0.0, high_ref[pl.ds(2 * comp, 2)])
        near = jnp.where(first, high, low)
        far = pltpu.roll(jnp.where(first, low, high), 124, axis=2)
        strip_ref[pl.ds(4 * comp, 2)] = near
        strip_ref[pl.ds(4 * comp + 2, 2)] = far
        up, down = pair_rows(near, far)
        up_ref[pl.ds(2 * comp, 2)] = up
        down_ref[pl.ds(2 * comp, 2)] = down


def table_of(eps_ref, sig_ref):
    keeps, drives = [], []
    one = jnp.ones((1, 256), F32)
    for index in range(MATS):
        eps = one * eps_ref[index]
        loss = (one * sig_ref[index]) / (2.0 * eps)
        keeps.append((1.0 - loss) / (1.0 + loss))
        drives.append(COURANT / (eps * (1.0 + loss)))
    return keeps, drives


def lookup(code, table):
    keep = jnp.zeros(code.shape, F32)
    drive = jnp.zeros(code.shape, F32)
    for index in range(MATS):
        chosen = code == index + 1.0
        keep = jnp.where(chosen, table[0][index], keep)
        drive = jnp.where(chosen, table[1][index], drive)
    return keep, drive


def wide(own, near_row, strip, corner, slot):
    turn = (128 - 8 * slot) % 128
    if turn:
        strip = pltpu.roll(strip, turn, axis=1)
        corner = pltpu.roll(corner, turn, axis=1)
    return jnp.concatenate(
        (jnp.concatenate((own, strip), axis=1), jnp.concatenate((near_row, corner), axis=1)), axis=0
    )


def ahead(field, axis):
    return pltpu.roll(field, field.shape[axis] - 1, axis=axis)


def behind(field, axis):
    return pltpu.roll(field, 1, axis=axis)


def magnetic(e, e_next, h, rate):
    ex, ey, ez = e
    new_x = h[0] - rate * (ahead(ez, 1) - ez - (e_next[1] - ey))
    new_y = h[1] - rate * (e_next[0] - ex - (ahead(ez, 0) - ez))
    new_z = h[2] - rate * (ahead(ey, 0) - ey - (ahead(ex, 1) - ex))
    return new_x, new_y, new_z


def electric(e, h, h_last, keep, drive):
    hx, hy, hz = h
    new_x = keep * e[0] + drive * (hz - behind(hz, 1) - (hy - h_last[1]))
    new_y = keep * e[1] + drive * (hx - h_last[0] - (hz - behind(hz, 0)))
    new_z = keep * e[2] + drive * (hy - behind(hy, 0) - (hx - behind(hx, 1)))
    return new_x, new_y, new_z


def near_kernel(
    own_ref, down_ref, high_ref, corner_ref, eps_ref, sig_ref, near_ref, info_ref
):
    fields = []
    for comp in range(7):
        layers = []
        for z in range(TOP):
            k = comp * TOP + z
            group, slot = divmod(k, 16)
            layers.append(
                wide(own_ref[k], down_ref[k], high_ref[group], corner_ref[group], slot)
            )
        fields.append(layers)
    e = [tuple(fields[c][z] for c in range(3)) for z in range(TOP)]
    h = [tuple(fields[c + 3][z] for c in range(3)) for z in range(TOP)]
    zero = jnp.zeros((16, 256), F32)
    table = table_of(eps_ref, sig_ref)
    coefs = [lookup(fields[6][z], table) for z in range(TOP)]
    last_x, last_y = at_end(GX, True), at_end(GY, True)
    row, lane = sub_iota((16, 256)), lane_iota((16, 256))

    def kept(flag, place, at):
        return 1.0 - (place == at).astype(F32) * flag.astype(F32)

    masks = {
        (0, 1): kept(last_x, row, 7), (1, 1): kept(last_y, lane, 127),
        (0, 0): kept(last_x, row, 8), (1, 0): kept(last_y, lane, 128),
    }

    def over(field, axis):
        return ahead(field, axis) * masks[axis, 1]

    def back(field, axis):
        return behind(field, axis) * masks[axis, 0]

    for step in range(STEPS):
        for z in range(step, TOP):
            ex, ey, ez = e[z]
            e_next = e[z + 1] if z + 1 < TOP else (zero, zero)
            h[z] = (
                h[z][0] - COURANT * (over(ez, 1) - ez - (e_next[1] - ey)),
                h[z][1] - COURANT * (e_next[0] - ex - (over(ez, 0) - ez)),
                h[z][2] - COURANT * (over(ey, 0) - ey - (over(ex, 1) - ex)),
            )
        for z in range(step + 1, TOP):
            keep, drive = coefs[z]
            hx, hy, hz = h[z]
            e[z] = (
                keep * e[z][0] + drive * (hz - back(hz, 1) - (hy - h[z - 1][1])),
                keep * e[z][1] + drive * (hx - h[z - 1][0] - (hz - back(hz, 0))),
                keep * e[z][2] + drive * (hy - back(hy, 0) - (hx - back(hx, 1))),
            )
    for pol in range(2):
        tile = pltpu.roll(pltpu.roll(e[TOP - 1][pol], 12, axis=0), 252, axis=1)
        near_ref[:, pol] = jnp.broadcast_to(tile[:8, :128].astype(BF16), (16, 8, 8, 128))
    lane = lane_iota((8, 128))
    info = own_ref[THIN - 1]
    for k, other in enumerate((high_ref[3], down_ref[THIN - 1], corner_ref[3])):
        info = jnp.where(lane < 8 * k + 8, info, pltpu.roll(other, 8 * k + 8, axis=1))
    info_ref[...] = info


def yee_kernel(
    e_ref, h_ref, mat_ref, up_ref, down_ref, strip_ref, cup_ref, cdown_ref, eps_ref, sig_ref,
    e_out, h_out, e_s, h_s, c_s,
):
    for comp in range(3):
        e_s[comp, NZ] = jnp.zeros((16, 256), F32)
        h_s[comp, 0] = jnp.zeros((16, 256), F32)
    no_up, no_down = at_end(GX, False), at_end(GX, True)
    for comp in range(7):
        near, far = unpair_rows(
            jnp.where(no_up, 0.0, up_ref[pl.ds(32 * comp, 32)]),
            jnp.where(no_down, 0.0, down_ref[pl.ds(32 * comp, 32)]),
        )
        edge = unpair_rows(
            jnp.where(no_up, 0.0, cup_ref[pl.ds(2 * comp, 2)]),
            jnp.where(no_down, 0.0, cdown_ref[pl.ds(2 * comp, 2)]),
        )
        for z in range(NZ):
            group, slot = divmod(z, 16)
            rows = near[z] if z < 32 else far[z - 32]
            own = thin_component(e_ref, h_ref, mat_ref, comp, z)
            value = wide(
                own, rows, strip_ref[4 * comp + group], edge[group // 2][group % 2], slot
            )
            if comp < 3:
                e_s[comp, z] = value
            elif comp < 6:
                h_s[comp - 3, z + 1] = value
            else:
                c_s[2, z] = value

    table = table_of(eps_ref, sig_ref)

    def coef(i, carry):
        for j in range(4):
            z = 4 * i + j
            code = c_s[2, z]
            keep, drive = lookup(code, table)
            c_s[0, z] = keep
            c_s[1, z] = drive
            c_s[2, z] = jnp.where(code > 0.5, COURANT, 0.0)
        return carry

    lax.fori_loop(0, NZ // 4, coef, 0)

    def step(k, carry):
        def block(i, carry):
            first = i * BLOCK
            for j in range(BLOCK):
                z = first + j
                e = tuple(e_s[c, z] for c in range(3))
                e_next = (e_s[0, z + 1], e_s[1, z + 1])
                h = tuple(h_s[c, z + 1] for c in range(3))
                h = magnetic(e, e_next, h, c_s[2, z])
                for c in range(3):
                    h_s[c, z + 1] = h[c]
            for j in range(BLOCK):
                z = first + j
                e = tuple(e_s[c, z] for c in range(3))
                h = tuple(h_s[c, z + 1] for c in range(3))
                e = electric(e, h, (h_s[0, z], h_s[1, z]), c_s[0, z], c_s[1, z])
                for c in range(3):
                    e_s[c, z] = e[c]
            return carry

        return lax.fori_loop(0, NZ // BLOCK, block, carry)

    lax.fori_loop(0, STEPS, step, 0)
    for comp in range(3):
        e_out[comp] = e_s[comp, pl.ds(0, NZ), pl.ds(0, 8), pl.ds(0, 128)]
        h_out[comp] = h_s[comp, pl.ds(1, NZ), pl.ds(0, 8), pl.ds(0, 128)]


def dot(a, b):
    return jnp.dot(a, b, preferred_element_type=F32)


def cut(ref, a, b):
    turn = (128 - b) % 128
    first = pltpu.roll(ref[0, pl.ds(a, PW), :], turn, axis=1)
    second = pltpu.roll(ref[1, pl.ds(a, PW), :], turn, axis=1)
    lane = lane_iota((PW, 128))
    return jnp.where(lane + b < 128, first, second)


def image_kernel(
    place_ref, info_ref, recv_ref, tyh_ref, tyl_ref, txh_ref, txl_ref, second_ref, first_ref,
    up_ref, mask_ref, after_ref, out_ref, near_s, re_s, im_s, half_s, acc_s,
):
    for j in range(8):
        tile = recv_ref[:, j].astype(F32).reshape(K, 128)
        near_s[pl.ds(K * (j // 4), K), pl.ds(128 * (j % 4), 128)] = tile.astype(BF16)
    near = near_s[...]
    both = dot(near, tyh_ref[...]) + dot(near, tyl_ref[...])
    half = both[:K] + jnp.where(lane_iota((1, 2 * K)) % 2 == 0, both[K:], -both[K:])
    half_h = half.astype(BF16)
    half_l = (half - half_h.astype(F32)).astype(BF16)
    blocks = dot(txh_ref[...], half_h) + (dot(txh_ref[...], half_l) + dot(txl_ref[...], half_h))
    scale = 1.0 / 512.0
    real = (blocks[:K, :K] + blocks[K:, K:]) * scale
    imag = (blocks[:K, K:] - blocks[K:, :K]) * scale
    real = real.astype(BF16).astype(F32)
    imag = imag.astype(BF16).astype(F32)
    for t in range(2):
        re_s[t] = real[:, 128 * t : 128 * t + 128]
        im_s[t] = imag[:, 128 * t : 128 * t + 128]
    mask = mask_ref[...].astype(F32)
    side = lax.axis_index("x") % 2

    def cuts(i, carry):
        for t in range(8):
            a = place_ref[t, 8 * i]
            b = place_ref[t, 8 * i + 1]
            window = jnp.concatenate(
                (cut(re_s, a, b) * mask, cut(im_s, a, b) * mask), axis=1
            ).astype(BF16)
            half = dot(window, second_ref[side]).astype(BF16)
            half_s[i, pl.ds(0, 128), pl.ds(128 * t, 128)] = half[:, :128]
            half_s[i, pl.ds(128, 128), pl.ds(128 * t, 128)] = half[:, 128:]
        return carry

    lax.fori_loop(0, 4, cuts, 0)
    acc_s[...] = jnp.zeros(acc_s.shape, F32)

    def fields(i, carry):
        field = dot(first_ref[...], half_s[i])
        power = field[:GRID] * field[:GRID] + field[GRID:] * field[GRID:]
        total = acc_s[...]
        for t in range(8):
            weight = info_ref[t, 8 * i + 2] * (1.0 / SOURCES)
            total = total + power[:, 128 * t : 128 * t + 128] * weight
        acc_s[...] = total
        return carry

    lax.fori_loop(0, 4, fields, 0)
    out_ref[...] = jnp.dot(
        up_ref[...], acc_s[...], precision=lax.Precision.HIGHEST, preferred_element_type=F32
    )


def sum_kernel(recv_ref, up_ref, out_ref):
    total = jnp.sum(recv_ref[...].reshape(64, 8, 128), axis=0)
    total = total + pltpu.roll(total, 4, axis=0)
    line = jnp.concatenate((total, pltpu.roll(total, 6, axis=0)), axis=1)
    full = lax.dot_general(
        line, up_ref[...], (((1,), (1,)), ((), ())), precision=lax.Precision.HIGHEST,
        preferred_element_type=F32,
    )
    out_ref[...] = full[:2]


def shifted(value, axes, by, cyclic=True):
    count = lax.axis_size(axes)
    pairs = [(i, (i + by) % count) for i in range(count)]
    if not cyclic:
        pairs = [(i, j) for i, j in pairs if j == i + by]
    return lax.ppermute(value, axes, pairs)


def diagonal(value):
    rows, cols = lax.axis_size(GX), lax.axis_size(GY)
    pairs = [
        (i * cols + j, (i - 1) % rows * cols + (j - 1) % cols)
        for i in range(rows)
        for j in range(cols)
    ]
    return lax.ppermute(value, ALL, pairs)


def local(
    e_field, h_field, material, permittivity, conductivity, src_shift, src_weight, pupil_mask
):
    rows_all = e_field.shape[2] * lax.axis_size(GX)
    cols_all = e_field.shape[3] * lax.axis_size(GY)
    tyh, tyl, txh, txl, second, first, upsample = map(jnp.asarray, tables(rows_all, cols_all))
    smem = pl.BlockSpec(memory_space=pltpu.SMEM)
    vmem = pl.BlockSpec(memory_space=pltpu.VMEM)

    params = pltpu.CompilerParams(vmem_limit_bytes=28 * 1024 * 1024)

    def here(value):
        return pltpu.with_memory_space_constraint(value, pltpu.VMEM)

    def far(value):
        return pltpu.with_memory_space_constraint(value, pltpu.HBM)

    def shape(*dims, dtype=F32):
        return jax.ShapeDtypeStruct(dims, dtype)

    field = pl.BlockSpec((3, 8, 8, 128), lambda i: (0, 7, 0, 0))
    layer = pl.BlockSpec((8, 8, 128), lambda i: (7, 0, 0))
    thin = pl.BlockSpec((THIN, 8, 128), lambda i: (0, 0, 0))
    head = pl.BlockSpec((4, 8, 128), lambda i: (0, 0, 0))
    thin_x, thin_y = pl.pallas_call(
        thin_kernel,
        grid=(1,),
        out_shape=(shape(THIN, 8, 128), shape(4, 8, 128)),
        in_specs=[field, field, layer, smem, smem],
        out_specs=(thin, head),
        compiler_params=params,
        name="thin",
    )(far(e_field), far(h_field), far(material), src_shift.T, src_weight)
    next_xy = diagonal(thin_y)
    next_y = shifted(thin_y, GY, -1)
    next_x = shifted(thin_x, GX, -1)
    near, info = pl.pallas_call(
        near_kernel,
        out_shape=(shape(16, 2, 8, 8, 128, dtype=BF16), shape(8, 128)),
        in_specs=[vmem] * 4 + [smem, smem],
        out_specs=(vmem, vmem),
        compiler_params=params,
        name="near",
    )(
        here(thin_x), here(next_x), here(next_y), here(next_xy), permittivity, conductivity
    )
    recv = lax.all_to_all(near.reshape(256, 8, 128), ALL, 0, 0, tiled=True)

    whole = [vmem, vmem, vmem, pl.BlockSpec(memory_space=pl.ANY)]
    to_low, to_high = pl.pallas_call(
        strip_kernel,
        out_shape=(shape(14, 8, 128), shape(14, 8, 128)),
        in_specs=whole,
        out_specs=(vmem, vmem),
        compiler_params=params,
        name="strip",
    )(e_field, h_field, material, thin_y)
    low = shifted(to_high, GY, 1)
    high = shifted(to_low, GY, -1)
    up, down = pl.pallas_call(
        rows_kernel,
        out_shape=(shape(224, 8, 128), shape(224, 8, 128)),
        in_specs=whole,
        out_specs=(vmem, vmem),
        compiler_params=params,
        name="rows",
    )(e_field, h_field, material, to_low)
    up_in = shifted(up, GX, 1, cyclic=False)
    down_in = shifted(down, GX, -1, cyclic=False)
    strip, cup, cdown = pl.pallas_call(
        corner_kernel,
        out_shape=(shape(28, 8, 128), shape(14, 8, 128), shape(14, 8, 128)),
        in_specs=[vmem] * 2,
        out_specs=(vmem,) * 3,
        compiler_params=params,
        name="corner",
    )(here(low), here(high))
    cup_in = shifted(cup, GX, 1)
    cdown_in = shifted(cdown, GX, -1)

    e_final, h_final = pl.pallas_call(
        yee_kernel,
        out_shape=(shape(*e_field.shape), shape(*h_field.shape)),
        in_specs=[vmem] * 8 + [smem, smem],
        out_specs=(vmem, vmem),
        scratch_shapes=[
            pltpu.VMEM((3, NZ + 1, 16, 256), F32),
            pltpu.VMEM((3, NZ + 1, 16, 256), F32),
            pltpu.VMEM((3, NZ, 16, 256), F32),
        ],
        cost_estimate=pl.CostEstimate(flops=40000000, transcendentals=0, bytes_accessed=8000000),
        compiler_params=params,
        name="yee",
    )(
        e_field, h_field, material, here(up_in), here(down_in), here(strip), here(cup_in),
        here(cdown_in), permittivity, conductivity,
    )

    partial = pl.pallas_call(
        image_kernel,
        out_shape=shape(2 * GRID, 128),
        in_specs=[smem, smem] + [vmem] * 9 + [pl.BlockSpec(memory_space=pl.ANY)],
        out_specs=vmem,
        scratch_shapes=[
            pltpu.VMEM((2 * K, 512), BF16),
            pltpu.VMEM((2, K, 128), F32),
            pltpu.VMEM((2, K, 128), F32),
            pltpu.VMEM((4, 256, 1024), BF16),
            pltpu.VMEM((GRID, 128), F32),
        ],
        compiler_params=params,
        name="image",
    )(
        info.astype(jnp.int32), info, here(recv.reshape(32, 8, 8, 128)), far(tyh), far(tyl),
        far(txh), far(txl), far(second), far(first), far(upsample), far(pupil_mask), cup,
    )
    pieces = lax.all_to_all(partial.reshape(256, 2, 128), ALL, 0, 0, tiled=True)
    image = pl.pallas_call(
        sum_kernel,
        out_shape=shape(2, IMG),
        in_specs=[vmem, vmem],
        out_specs=vmem,
        compiler_params=params,
        name="total",
    )(here(pieces.reshape(512, 128)), far(upsample))
    return image, e_final, h_final


def solution(mesh):
    finer = Mesh(mesh.devices.reshape(4, 4, 2, 2, 4), ALL)
    return jax.shard_map(
        local,
        mesh=finer,
        in_specs=(
            P(None, None, GX, GY),
            P(None, None, GX, GY),
            P(None, GX, GY),
            P(),
            P(),
            P(ALL, None),
            P(ALL),
            P(),
        ),
        out_specs=(P(ALL, None), P(None, None, GX, GY), P(None, None, GX, GY)),
        check_vma=False,
    )
```

```python
import math

import numpy as np
import jax
import jax.numpy as jnp
from jax import lax
from jax.experimental import pallas as pl
from jax.experimental.pallas import tpu as pltpu
from jax.sharding import Mesh
from jax.sharding import PartitionSpec as P


STEPS = 4
COURANT = 0.5
NZ = 64
K = 256
PW = 128
IMG = 512
GRID = IMG // 2
MATS = 8
SOURCES = 2048
TOP = 5
BLOCK = 16
THIN = 36
GX = ("zl", "y", "c")
GY = ("zh", "x")
ALL = GX + GY
F32 = jnp.float32
BF16 = jnp.bfloat16


def split_bf16(table):
    high = table.astype(np.float32).astype(jnp.bfloat16)
    low = (table - high.astype(np.float64)).astype(np.float32).astype(jnp.bfloat16)
    return high, low


def cosine_basis():
    orders, places = np.arange(128)[:, None], np.arange(128)[None, :]
    basis = np.cos(np.pi * orders * (2 * places + 1) / 256) * math.sqrt(2.0 / 128)
    basis[0] *= math.sqrt(0.5)
    return basis


def tables(rows_all, cols_all):
    freqs = np.arange(K) - K // 2
    phase_y = 2.0 * np.pi * (np.outer(np.arange(cols_all // 2) + STEPS, freqs) % cols_all) / cols_all
    ty = np.concatenate((np.cos(phase_y), -np.sin(phase_y)), axis=1)
    code = cosine_basis()
    ty = np.concatenate([code @ ty[k : k + 128] for k in range(0, ty.shape[0], 128)])
    phase_x = 2.0 * np.pi * (np.outer(freqs, np.arange(rows_all) + STEPS) % rows_all) / rows_all
    tx = np.concatenate((np.cos(phase_x), np.sin(phase_x)), axis=0)
    offsets = np.arange(PW) - PW // 2
    places = 2 * np.arange(GRID)
    phase = 2.0 * np.pi * (np.outer(offsets, places) % IMG) / IMG
    cosine, sine = np.cos(phase), np.sin(phase)
    seconds = []
    for half in range(2):
        c = cosine[:, half * 128 : half * 128 + 128]
        s = sine[:, half * 128 : half * 128 + 128]
        seconds.append(np.concatenate((np.concatenate((c, s), 1), np.concatenate((-s, c), 1)), 0))
    second = np.stack(seconds).astype(np.float32).astype(jnp.bfloat16)
    rc, rs = cosine.T / PW, sine.T / PW
    first = np.concatenate((np.concatenate((rc, -rs), 1), np.concatenate((rs, rc), 1)), 0)
    first = first.astype(np.float32).astype(jnp.bfloat16)
    lag = np.arange(-IMG, IMG + 1)
    orders = np.arange(1, GRID // 2)
    kernel = 1.0 + 2.0 * np.cos(2.0 * np.pi * np.outer(lag, orders) / IMG).sum(1)
    kernel = (kernel + np.cos(2.0 * np.pi * (GRID // 2) * lag / IMG)) / GRID
    between = np.arange(IMG)[:, None] - 2 * np.arange(GRID)[None, :]
    upsample = kernel[between + IMG]
    upsample[::2] = np.eye(GRID)
    return split_bf16(ty) + split_bf16(tx) + (second, first, upsample.astype(np.float32))


def sub_iota(shape):
    return lax.broadcasted_iota(jnp.int32, shape, len(shape) - 2)


def lane_iota(shape):
    return lax.broadcasted_iota(jnp.int32, shape, len(shape) - 1)


def pair_rows(near, far):
    turned = pltpu.roll(far, 4, axis=far.ndim - 2)
    low = sub_iota(near.shape) < 4
    return jnp.where(low, turned, near), jnp.where(low, near, turned)


def unpair_rows(up, down):
    low = sub_iota(up.shape) < 4
    near = jnp.where(low, down, up)
    far = pltpu.roll(jnp.where(low, up, down), 4, axis=up.ndim - 2)
    return near, far


def component(e_ref, h_ref, mat_ref, comp):
    if comp < 3:
        return e_ref[comp]
    if comp < 6:
        return h_ref[comp - 3]
    return (mat_ref[...] + 1).astype(F32)


def thin_component(e_ref, h_ref, mat_ref, comp, z):
    if comp < 3:
        return e_ref[comp, z]
    if comp < 6:
        return h_ref[comp - 3, z]
    return (mat_ref[z] + 1).astype(F32)


def packed_strip(block):
    slot = (lane_iota((4, 8, 128)) + 4) // 8 % 16
    layers = block.reshape(4, 16, 8, 128)
    strip = layers[:, 0]
    for s in range(1, 16):
        strip = jnp.where(slot == s, pltpu.roll(layers[:, s], 8 * s, axis=2), strip)
    return strip[:2], pltpu.roll(strip[2:], 4, axis=2)


def thin_kernel(e_ref, h_ref, mat_ref, shift_ref, weight_ref, down_ref, low_ref):
    slot = lane_iota((8, 128)) // 8
    thin = []
    for comp in range(7):
        for z in range(8 - TOP, 8):
            thin.append(thin_component(e_ref, h_ref, mat_ref, comp, z))
    for k, tile in enumerate(thin):
        down_ref[k] = tile
    for g in range(3):
        strip = thin[16 * g]
        for s, tile in enumerate(thin[16 * g + 1 : 16 * g + 16]):
            strip = jnp.where(slot == s + 1, pltpu.roll(tile, 8 * (s + 1), axis=1), strip)
        low_ref[g] = strip
    row = sub_iota((8, 128))
    lane = lane_iota((8, 128))
    info = jnp.zeros((8, 128), F32)
    for s in range(8):
        here = row == s
        info = jnp.where(here & (lane == 0), shift_ref[0, s].astype(F32), info)
        info = jnp.where(here & (lane == 1), shift_ref[1, s].astype(F32), info)
        info = jnp.where(here & (lane == 2), weight_ref[s], info)
    down_ref[THIN - 1] = info
    low_ref[3] = info


def strip_kernel(e_ref, h_ref, mat_ref, after_ref, low_ref, high_ref):
    first = lane_iota((2, 8, 128)) % 8 < 4
    for comp in range(7):
        near, far = packed_strip(component(e_ref, h_ref, mat_ref, comp))
        low_ref[pl.ds(2 * comp, 2)] = jnp.where(first, near, far)
        high_ref[pl.ds(2 * comp, 2)] = jnp.where(first, far, near)


def rows_kernel(e_ref, h_ref, mat_ref, after_ref, up_ref, down_ref):
    for comp in range(7):
        block = component(e_ref, h_ref, mat_ref, comp)
        up, down = pair_rows(block[:32], block[32:])
        up_ref[pl.ds(32 * comp, 32)] = up
        down_ref[pl.ds(32 * comp, 32)] = down


def at_end(axes, last):
    flag = None
    for axis in axes:
        here = lax.axis_index(axis) == (lax.axis_size(axis) - 1 if last else 0)
        flag = here if flag is None else flag & here
    return flag


def corner_kernel(low_ref, high_ref, strip_ref, up_ref, down_ref):
    first = lane_iota((2, 8, 128)) % 8 < 4
    no_low, no_high = at_end(GY, False), at_end(GY, True)
    for comp in range(7):
        low = jnp.where(no_low, 0.0, low_ref[pl.ds(2 * comp, 2)])
        high = jnp.where(no_high, 0.0, high_ref[pl.ds(2 * comp, 2)])
        near = jnp.where(first, high, low)
        far = pltpu.roll(jnp.where(first, low, high), 124, axis=2)
        strip_ref[pl.ds(4 * comp, 2)] = near
        strip_ref[pl.ds(4 * comp + 2, 2)] = far
        up, down = pair_rows(near, far)
        up_ref[pl.ds(2 * comp, 2)] = up
        down_ref[pl.ds(2 * comp, 2)] = down


def table_of(eps_ref, sig_ref):
    keeps, drives = [], []
    one = jnp.ones((1, 256), F32)
    for index in range(MATS):
        eps = one * eps_ref[index]
        loss = (one * sig_ref[index]) / (2.0 * eps)
        keeps.append((1.0 - loss) / (1.0 + loss))
        drives.append(COURANT / (eps * (1.0 + loss)))
    return keeps, drives


def lookup(code, table):
    keep = jnp.zeros(code.shape, F32)
    drive = jnp.zeros(code.shape, F32)
    for index in range(MATS):
        chosen = code == index + 1.0
        keep = jnp.where(chosen, table[0][index], keep)
        drive = jnp.where(chosen, table[1][index], drive)
    return keep, drive


def wide(own, near_row, strip, corner, slot):
    turn = (128 - 8 * slot) % 128
    if turn:
        strip = pltpu.roll(strip, turn, axis=1)
        corner = pltpu.roll(corner, turn, axis=1)
    return jnp.concatenate(
        (jnp.concatenate((own, strip), axis=1), jnp.concatenate((near_row, corner), axis=1)), axis=0
    )


def ahead(field, axis):
    return pltpu.roll(field, field.shape[axis] - 1, axis=axis)


def behind(field, axis):
    return pltpu.roll(field, 1, axis=axis)


def magnetic(e, e_next, h, rate):
    ex, ey, ez = e
    new_x = h[0] - rate * (ahead(ez, 1) - ez - (e_next[1] - ey))
    new_y = h[1] - rate * (e_next[0] - ex - (ahead(ez, 0) - ez))
    new_z = h[2] - rate * (ahead(ey, 0) - ey - (ahead(ex, 1) - ex))
    return new_x, new_y, new_z


def electric(e, h, h_last, keep, drive):
    hx, hy, hz = h
    new_x = keep * e[0] + drive * (hz - behind(hz, 1) - (hy - h_last[1]))
    new_y = keep * e[1] + drive * (hx - h_last[0] - (hz - behind(hz, 0)))
    new_z = keep * e[2] + drive * (hy - behind(hy, 0) - (hx - behind(hx, 1)))
    return new_x, new_y, new_z


def near_kernel(
    own_ref, down_ref, high_ref, corner_ref, code_ref, eps_ref, sig_ref, near_ref, info_ref
):
    fields = []
    for comp in range(7):
        layers = []
        for z in range(TOP):
            k = comp * TOP + z
            group, slot = divmod(k, 16)
            layers.append(
                wide(own_ref[k], down_ref[k], high_ref[group], corner_ref[group], slot)
            )
        fields.append(layers)
    e = [tuple(fields[c][z] for c in range(3)) for z in range(TOP)]
    h = [tuple(fields[c + 3][z] for c in range(3)) for z in range(TOP)]
    zero = jnp.zeros((16, 256), F32)
    table = table_of(eps_ref, sig_ref)
    coefs = [lookup(fields[6][z], table) for z in range(TOP)]
    last_x, last_y = at_end(GX, True), at_end(GY, True)
    row, lane = sub_iota((16, 256)), lane_iota((16, 256))

    def kept(flag, place, at):
        return 1.0 - (place == at).astype(F32) * flag.astype(F32)

    masks = {
        (0, 1): kept(last_x, row, 7), (1, 1): kept(last_y, lane, 127),
        (0, 0): kept(last_x, row, 8), (1, 0): kept(last_y, lane, 128),
    }

    def over(field, axis):
        return ahead(field, axis) * masks[axis, 1]

    def back(field, axis):
        return behind(field, axis) * masks[axis, 0]

    for step in range(STEPS):
        for z in range(step, TOP):
            ex, ey, ez = e[z]
            e_next = e[z + 1] if z + 1 < TOP else (zero, zero)
            h[z] = (
                h[z][0] - COURANT * (over(ez, 1) - ez - (e_next[1] - ey)),
                h[z][1] - COURANT * (e_next[0] - ex - (over(ez, 0) - ez)),
                h[z][2] - COURANT * (over(ey, 0) - ey - (over(ex, 1) - ex)),
            )
        for z in range(step + 1, TOP):
            keep, drive = coefs[z]
            hx, hy, hz = h[z]
            e[z] = (
                keep * e[z][0] + drive * (hz - back(hz, 1) - (hy - h[z - 1][1])),
                keep * e[z][1] + drive * (hx - h[z - 1][0] - (hz - back(hz, 0))),
                keep * e[z][2] + drive * (hy - back(hy, 0) - (hx - back(hx, 1))),
            )
    tiles = []
    for pol in range(2):
        tile = pltpu.roll(pltpu.roll(e[TOP - 1][pol], 12, axis=0), 252, axis=1)
        tiles.append(tile[:8, :128])
    coded = jnp.dot(
        jnp.concatenate(tiles, axis=0), code_ref[...], precision=lax.Precision.HIGHEST,
        preferred_element_type=F32,
    ).astype(BF16)
    for pol in range(2):
        near_ref[:, pol] = jnp.broadcast_to(coded[8 * pol : 8 * pol + 8], (16, 8, 8, 128))
    lane = lane_iota((8, 128))
    info = own_ref[THIN - 1]
    for k, other in enumerate((high_ref[3], down_ref[THIN - 1], corner_ref[3])):
        info = jnp.where(lane < 8 * k + 8, info, pltpu.roll(other, 8 * k + 8, axis=1))
    info_ref[...] = info


def yee_kernel(
    e_ref, h_ref, mat_ref, up_ref, down_ref, strip_ref, cup_ref, cdown_ref, eps_ref, sig_ref,
    e_out, h_out, e_s, h_s, c_s,
):
    for comp in range(3):
        e_s[comp, NZ] = jnp.zeros((16, 256), F32)
        h_s[comp, 0] = jnp.zeros((16, 256), F32)
    no_up, no_down = at_end(GX, False), at_end(GX, True)
    for comp in range(7):
        near, far = unpair_rows(
            jnp.where(no_up, 0.0, up_ref[pl.ds(32 * comp, 32)]),
            jnp.where(no_down, 0.0, down_ref[pl.ds(32 * comp, 32)]),
        )
        edge = unpair_rows(
            jnp.where(no_up, 0.0, cup_ref[pl.ds(2 * comp, 2)]),
            jnp.where(no_down, 0.0, cdown_ref[pl.ds(2 * comp, 2)]),
        )
        for z in range(NZ):
            group, slot = divmod(z, 16)
            rows = near[z] if z < 32 else far[z - 32]
            own = thin_component(e_ref, h_ref, mat_ref, comp, z)
            value = wide(
                own, rows, strip_ref[4 * comp + group], edge[group // 2][group % 2], slot
            )
            if comp < 3:
                e_s[comp, z] = value
            elif comp < 6:
                h_s[comp - 3, z + 1] = value
            else:
                c_s[2, z] = value

    table = table_of(eps_ref, sig_ref)

    def coef(i, carry):
        for j in range(4):
            z = 4 * i + j
            code = c_s[2, z]
            keep, drive = lookup(code, table)
            c_s[0, z] = keep
            c_s[1, z] = drive
            c_s[2, z] = jnp.where(code > 0.5, COURANT, 0.0)
        return carry

    lax.fori_loop(0, NZ // 4, coef, 0)

    def advance_h(z):
        e = tuple(e_s[c, z] for c in range(3))
        e_next = (e_s[0, z + 1], e_s[1, z + 1])
        h = tuple(h_s[c, z + 1] for c in range(3))
        h = magnetic(e, e_next, h, c_s[2, z])
        for c in range(3):
            h_s[c, z + 1] = h[c]
        return h

    def advance_e(z):
        e = tuple(e_s[c, z] for c in range(3))
        h = tuple(h_s[c, z + 1] for c in range(3))
        return electric(e, h, (h_s[0, z], h_s[1, z]), c_s[0, z], c_s[1, z])

    def step(k, carry):
        def block(i, carry):
            first = i * BLOCK
            for j in range(BLOCK):
                advance_h(first + j)
            for j in range(BLOCK):
                z = first + j
                e = advance_e(z)
                for c in range(3):
                    e_s[c, z] = e[c]
            return carry

        return lax.fori_loop(0, NZ // BLOCK, block, carry)

    lax.fori_loop(0, STEPS - 1, step, 0)

    def final(i, carry):
        first = i * BLOCK
        for j in range(BLOCK):
            z = first + j
            h = advance_h(z)
            for c in range(3):
                h_out[c, z] = h[c][:8, :128]
        for j in range(BLOCK):
            z = first + j
            e = advance_e(z)
            for c in range(3):
                e_out[c, z] = e[c][:8, :128]
        return carry

    lax.fori_loop(0, NZ // BLOCK, final, 0)


def dot(a, b):
    return jnp.dot(a, b, preferred_element_type=F32)


def cut(ref, a, b):
    turn = (128 - b) % 128
    first = pltpu.roll(ref[0, pl.ds(a, PW), :], turn, axis=1)
    second = pltpu.roll(ref[1, pl.ds(a, PW), :], turn, axis=1)
    lane = lane_iota((PW, 128))
    return jnp.where(lane + b < 128, first, second)


def image_kernel(
    place_ref, info_ref, recv_ref, tyh_ref, tyl_ref, txh_ref, txl_ref, second_ref, first_ref,
    up_ref, mask_ref, out_ref, near_s, re_s, im_s, win_s, half_s, acc_s,
):
    for j in range(8):
        tile = recv_ref[:, j].astype(F32).reshape(K, 128)
        near_s[pl.ds(K * (j // 4), K), pl.ds(128 * (j % 4), 128)] = tile.astype(BF16)
    near = near_s[...]
    both = dot(near, tyh_ref[...]) + dot(near, tyl_ref[...])
    half = both[:K] + jnp.where(lane_iota((1, 2 * K)) % 2 == 0, both[K:], -both[K:])
    half_h = half.astype(BF16)
    half_l = (half - half_h.astype(F32)).astype(BF16)
    blocks = dot(txh_ref[...], half_h) + (dot(txh_ref[...], half_l) + dot(txl_ref[...], half_h))
    scale = 1.0 / 512.0
    real = (blocks[:K, :K] + blocks[K:, K:]) * scale
    imag = (blocks[:K, K:] - blocks[K:, :K]) * scale
    real = real.astype(BF16).astype(F32)
    imag = imag.astype(BF16).astype(F32)
    for t in range(2):
        re_s[t] = real[:, 128 * t : 128 * t + 128]
        im_s[t] = imag[:, 128 * t : 128 * t + 128]
    mask = mask_ref[...].astype(F32)
    side = lax.axis_index("x") % 2

    def cuts(i, carry):
        for t in range(8):
            a = place_ref[t, 8 * i]
            b = place_ref[t, 8 * i + 1]
            window = jnp.concatenate(
                (cut(re_s, a, b) * mask, cut(im_s, a, b) * mask), axis=1
            ).astype(BF16)
            win_s[pl.ds(PW * t, PW)] = window
        half = dot(win_s[...], second_ref[side]).astype(BF16)
        for t in range(8):
            rows = half[PW * t : PW * t + PW]
            half_s[i, pl.ds(0, 128), pl.ds(128 * t, 128)] = rows[:, :128]
            half_s[i, pl.ds(128, 128), pl.ds(128 * t, 128)] = rows[:, 128:]
        return carry

    lax.fori_loop(0, 4, cuts, 0)
    acc_s[...] = jnp.zeros(acc_s.shape, F32)

    def fields(i, carry):
        field = dot(first_ref[...], half_s[i])
        power = field[:GRID] * field[:GRID] + field[GRID:] * field[GRID:]
        total = acc_s[...]
        for t in range(8):
            weight = info_ref[t, 8 * i + 2] * (1.0 / SOURCES)
            total = total + power[:, 128 * t : 128 * t + 128] * weight
        acc_s[...] = total
        return carry

    lax.fori_loop(0, 4, fields, 0)
    out_ref[...] = jnp.dot(
        up_ref[...], acc_s[...], precision=lax.Precision.HIGHEST, preferred_element_type=F32
    )


def sum_kernel(recv_ref, up_ref, out_ref):
    total = jnp.sum(recv_ref[...].reshape(64, 8, 128), axis=0)
    total = total + pltpu.roll(total, 4, axis=0)
    line = jnp.concatenate((total, pltpu.roll(total, 6, axis=0)), axis=1)
    full = lax.dot_general(
        line, up_ref[...], (((1,), (1,)), ((), ())), precision=lax.Precision.HIGHEST,
        preferred_element_type=F32,
    )
    out_ref[...] = full[:2]


def shifted(value, axes, by, cyclic=True):
    count = lax.axis_size(axes)
    pairs = [(i, (i + by) % count) for i in range(count)]
    if not cyclic:
        pairs = [(i, j) for i, j in pairs if j == i + by]
    return lax.ppermute(value, axes, pairs)


def diagonal(value):
    rows, cols = lax.axis_size(GX), lax.axis_size(GY)
    pairs = [
        (i * cols + j, (i - 1) % rows * cols + (j - 1) % cols)
        for i in range(rows)
        for j in range(cols)
    ]
    return lax.ppermute(value, ALL, pairs)


def local(
    e_field, h_field, material, permittivity, conductivity, src_shift, src_weight, pupil_mask
):
    rows_all = e_field.shape[2] * lax.axis_size(GX)
    cols_all = e_field.shape[3] * lax.axis_size(GY)
    tyh, tyl, txh, txl, second, first, upsample = map(jnp.asarray, tables(rows_all, cols_all))
    smem = pl.BlockSpec(memory_space=pltpu.SMEM)
    vmem = pl.BlockSpec(memory_space=pltpu.VMEM)

    params = pltpu.CompilerParams(vmem_limit_bytes=28 * 1024 * 1024)

    def here(value):
        return pltpu.with_memory_space_constraint(value, pltpu.VMEM)

    def far(value):
        return pltpu.with_memory_space_constraint(value, pltpu.HBM)

    def shape(*dims, dtype=F32):
        return jax.ShapeDtypeStruct(dims, dtype)

    field = pl.BlockSpec((3, 8, 8, 128), lambda i: (0, 7, 0, 0))
    layer = pl.BlockSpec((8, 8, 128), lambda i: (7, 0, 0))
    thin = pl.BlockSpec((THIN, 8, 128), lambda i: (0, 0, 0))
    head = pl.BlockSpec((4, 8, 128), lambda i: (0, 0, 0))
    thin_x, thin_y = pl.pallas_call(
        thin_kernel,
        grid=(1,),
        out_shape=(shape(THIN, 8, 128), shape(4, 8, 128)),
        in_specs=[field, field, layer, smem, smem],
        out_specs=(thin, head),
        compiler_params=params,
        name="thin",
    )(far(e_field), far(h_field), far(material), src_shift.T, src_weight)
    next_xy = diagonal(thin_y)
    next_y = shifted(thin_y, GY, -1)
    next_x = shifted(thin_x, GX, -1)
    near, info = pl.pallas_call(
        near_kernel,
        out_shape=(shape(16, 2, 8, 8, 128, dtype=BF16), shape(8, 128)),
        in_specs=[vmem] * 5 + [smem, smem],
        out_specs=(vmem, vmem),
        compiler_params=params,
        name="near",
    )(
        here(thin_x), here(next_x), here(next_y), here(next_xy),
        here(jnp.asarray(cosine_basis().T.astype(np.float32))), permittivity, conductivity,
    )
    recv = lax.all_to_all(near.reshape(256, 8, 128), ALL, 0, 0, tiled=True)

    whole = [vmem, vmem, vmem, pl.BlockSpec(memory_space=pl.ANY)]
    to_low, to_high = pl.pallas_call(
        strip_kernel,
        out_shape=(shape(14, 8, 128), shape(14, 8, 128)),
        in_specs=whole,
        out_specs=(vmem, vmem),
        compiler_params=params,
        name="strip",
    )(e_field, h_field, material, thin_y)
    low = shifted(to_high, GY, 1)
    high = shifted(to_low, GY, -1)
    up, down = pl.pallas_call(
        rows_kernel,
        out_shape=(shape(224, 8, 128), shape(224, 8, 128)),
        in_specs=whole,
        out_specs=(vmem, vmem),
        compiler_params=params,
        name="rows",
    )(e_field, h_field, material, to_low)
    up_in = shifted(up, GX, 1, cyclic=False)
    down_in = shifted(down, GX, -1, cyclic=False)
    strip, cup, cdown = pl.pallas_call(
        corner_kernel,
        out_shape=(shape(28, 8, 128), shape(14, 8, 128), shape(14, 8, 128)),
        in_specs=[vmem] * 2,
        out_specs=(vmem,) * 3,
        compiler_params=params,
        name="corner",
    )(here(low), here(high))
    cup_in = shifted(cup, GX, 1)
    cdown_in = shifted(cdown, GX, -1)

    e_final, h_final = pl.pallas_call(
        yee_kernel,
        out_shape=(shape(*e_field.shape), shape(*h_field.shape)),
        in_specs=[vmem] * 8 + [smem, smem],
        out_specs=(vmem, vmem),
        scratch_shapes=[
            pltpu.VMEM((3, NZ + 1, 16, 256), F32),
            pltpu.VMEM((3, NZ + 1, 16, 256), F32),
            pltpu.VMEM((3, NZ, 16, 256), F32),
        ],
        cost_estimate=pl.CostEstimate(flops=40000000, transcendentals=0, bytes_accessed=8000000),
        compiler_params=params,
        name="yee",
    )(
        e_field, h_field, material, here(up_in), here(down_in), here(strip), here(cup_in),
        here(cdown_in), permittivity, conductivity,
    )

    partial = pl.pallas_call(
        image_kernel,
        out_shape=shape(2 * GRID, 128),
        in_specs=[smem, smem] + [vmem] * 9,
        out_specs=vmem,
        scratch_shapes=[
            pltpu.VMEM((2 * K, 512), BF16),
            pltpu.VMEM((2, K, 128), F32),
            pltpu.VMEM((2, K, 128), F32),
            pltpu.VMEM((8 * PW, 256), BF16),
            pltpu.VMEM((4, 256, 1024), BF16),
            pltpu.VMEM((GRID, 128), F32),
        ],
        compiler_params=params,
        name="image",
    )(
        info.astype(jnp.int32), info, here(recv.reshape(32, 8, 8, 128)), far(tyh), far(tyl),
        far(txh), far(txl), far(second), far(first), far(upsample), far(pupil_mask),
    )
    pieces = lax.all_to_all(partial.reshape(256, 2, 128), ALL, 0, 0, tiled=True)
    image = pl.pallas_call(
        sum_kernel,
        out_shape=shape(2, IMG),
        in_specs=[vmem, vmem],
        out_specs=vmem,
        compiler_params=params,
        name="total",
    )(here(pieces.reshape(512, 128)), here(upsample))
    return image, e_final, h_final


def solution(mesh):
    finer = Mesh(mesh.devices.reshape(4, 4, 2, 2, 4), ALL)
    return jax.shard_map(
        local,
        mesh=finer,
        in_specs=(
            P(None, None, GX, GY),
            P(None, None, GX, GY),
            P(None, GX, GY),
            P(),
            P(),
            P(ALL, None),
            P(ALL),
            P(),
        ),
        out_specs=(P(ALL, None), P(None, None, GX, GY), P(None, None, GX, GY)),
        check_vma=False,
    )
```

```python
import math

import numpy as np
import jax
import jax.numpy as jnp
from jax import lax
from jax.experimental import pallas as pl
from jax.experimental.pallas import tpu as pltpu
from jax.sharding import Mesh
from jax.sharding import PartitionSpec as P


STEPS = 4
COURANT = 0.5
NZ = 64
K = 256
PW = 128
IMG = 512
GRID = IMG // 2
MATS = 8
SOURCES = 2048
TOP = 5
BLOCK = 16
THIN = 36
GX = ("zl", "y", "c")
GY = ("zh", "x")
ALL = GX + GY
F32 = jnp.float32
BF16 = jnp.bfloat16


def split_bf16(table):
    high = table.astype(np.float32).astype(jnp.bfloat16)
    low = (table - high.astype(np.float64)).astype(np.float32).astype(jnp.bfloat16)
    return high, low


def cosine_basis():
    orders, places = np.arange(128)[:, None], np.arange(128)[None, :]
    basis = np.cos(np.pi * orders * (2 * places + 1) / 256) * math.sqrt(2.0 / 128)
    basis[0] *= math.sqrt(0.5)
    return basis


def tables(rows_all, cols_all):
    freqs = np.arange(K) - K // 2
    phase_y = 2.0 * np.pi * (np.outer(np.arange(cols_all // 2) + STEPS, freqs) % cols_all) / cols_all
    ty = np.concatenate((np.cos(phase_y), -np.sin(phase_y)), axis=1)
    code = cosine_basis()
    ty = np.concatenate([code @ ty[k : k + 128] for k in range(0, ty.shape[0], 128)])
    phase_x = 2.0 * np.pi * (np.outer(freqs, np.arange(rows_all) + STEPS) % rows_all) / rows_all
    tx = np.concatenate((np.cos(phase_x), np.sin(phase_x)), axis=0)
    offsets = np.arange(PW) - PW // 2
    places = 2 * np.arange(GRID)
    phase = 2.0 * np.pi * (np.outer(offsets, places) % IMG) / IMG
    cosine, sine = np.cos(phase), np.sin(phase)
    seconds = []
    for half in range(2):
        c = cosine[:, half * 128 : half * 128 + 128]
        s = sine[:, half * 128 : half * 128 + 128]
        seconds.append(np.concatenate((np.concatenate((c, s), 1), np.concatenate((-s, c), 1)), 0))
    second = np.stack(seconds).astype(np.float32).astype(jnp.bfloat16)
    rc, rs = cosine.T / PW, sine.T / PW
    first = np.concatenate((np.concatenate((rc, -rs), 1), np.concatenate((rs, rc), 1)), 0)
    first = first.astype(np.float32).astype(jnp.bfloat16)
    lag = np.arange(-IMG, IMG + 1)
    orders = np.arange(1, GRID // 2)
    kernel = 1.0 + 2.0 * np.cos(2.0 * np.pi * np.outer(lag, orders) / IMG).sum(1)
    kernel = (kernel + np.cos(2.0 * np.pi * (GRID // 2) * lag / IMG)) / GRID
    between = np.arange(IMG)[:, None] - 2 * np.arange(GRID)[None, :]
    upsample = kernel[between + IMG]
    upsample[::2] = np.eye(GRID)
    return split_bf16(ty) + split_bf16(tx) + (second, first, upsample.astype(np.float32))


def sub_iota(shape):
    return lax.broadcasted_iota(jnp.int32, shape, len(shape) - 2)


def lane_iota(shape):
    return lax.broadcasted_iota(jnp.int32, shape, len(shape) - 1)


def pair_rows(near, far):
    turned = pltpu.roll(far, 4, axis=far.ndim - 2)
    low = sub_iota(near.shape) < 4
    return jnp.where(low, turned, near), jnp.where(low, near, turned)


def unpair_rows(up, down):
    low = sub_iota(up.shape) < 4
    near = jnp.where(low, down, up)
    far = pltpu.roll(jnp.where(low, up, down), 4, axis=up.ndim - 2)
    return near, far


def component(e_ref, h_ref, mat_ref, comp):
    if comp < 3:
        return e_ref[comp]
    if comp < 6:
        return h_ref[comp - 3]
    return (mat_ref[...] + 1).astype(F32)


def thin_component(e_ref, h_ref, mat_ref, comp, z):
    if comp < 3:
        return e_ref[comp, z]
    if comp < 6:
        return h_ref[comp - 3, z]
    return (mat_ref[z] + 1).astype(F32)


def packed_strip(block):
    slot = (lane_iota((4, 8, 128)) + 4) // 8 % 16
    layers = block.reshape(4, 16, 8, 128)
    strip = layers[:, 0]
    for s in range(1, 16):
        strip = jnp.where(slot == s, pltpu.roll(layers[:, s], 8 * s, axis=2), strip)
    return strip[:2], pltpu.roll(strip[2:], 4, axis=2)


def thin_kernel(e_ref, h_ref, mat_ref, shift_ref, weight_ref, down_ref, low_ref):
    slot = lane_iota((8, 128)) // 8
    thin = []
    for comp in range(7):
        for z in range(8 - TOP, 8):
            thin.append(thin_component(e_ref, h_ref, mat_ref, comp, z))
    for k, tile in enumerate(thin):
        down_ref[k] = tile
    for g in range(3):
        strip = thin[16 * g]
        for s, tile in enumerate(thin[16 * g + 1 : 16 * g + 16]):
            strip = jnp.where(slot == s + 1, pltpu.roll(tile, 8 * (s + 1), axis=1), strip)
        low_ref[g] = strip
    row = sub_iota((8, 128))
    lane = lane_iota((8, 128))
    info = jnp.zeros((8, 128), F32)
    for s in range(8):
        here = row == s
        info = jnp.where(here & (lane == 0), shift_ref[0, s].astype(F32), info)
        info = jnp.where(here & (lane == 1), shift_ref[1, s].astype(F32), info)
        info = jnp.where(here & (lane == 2), weight_ref[s], info)
    down_ref[THIN - 1] = info
    low_ref[3] = info


def strip_kernel(e_ref, h_ref, mat_ref, after_ref, low_ref, high_ref):
    first = lane_iota((2, 8, 128)) % 8 < 4
    for comp in range(7):
        near, far = packed_strip(component(e_ref, h_ref, mat_ref, comp))
        low_ref[pl.ds(2 * comp, 2)] = jnp.where(first, near, far)
        high_ref[pl.ds(2 * comp, 2)] = jnp.where(first, far, near)


def rows_kernel(e_ref, h_ref, mat_ref, after_ref, up_ref, down_ref):
    for comp in range(7):
        block = component(e_ref, h_ref, mat_ref, comp)
        up, down = pair_rows(block[:32], block[32:])
        up_ref[pl.ds(32 * comp, 32)] = up
        down_ref[pl.ds(32 * comp, 32)] = down


def at_end(axes, last):
    flag = None
    for axis in axes:
        here = lax.axis_index(axis) == (lax.axis_size(axis) - 1 if last else 0)
        flag = here if flag is None else flag & here
    return flag


def corner_kernel(low_ref, high_ref, strip_ref, up_ref, down_ref):
    first = lane_iota((2, 8, 128)) % 8 < 4
    no_low, no_high = at_end(GY, False), at_end(GY, True)
    for comp in range(7):
        low = jnp.where(no_low, 0.0, low_ref[pl.ds(2 * comp, 2)])
        high = jnp.where(no_high, 0.0, high_ref[pl.ds(2 * comp, 2)])
        near = jnp.where(first, high, low)
        far = pltpu.roll(jnp.where(first, low, high), 124, axis=2)
        strip_ref[pl.ds(4 * comp, 2)] = near
        strip_ref[pl.ds(4 * comp + 2, 2)] = far
        up, down = pair_rows(near, far)
        up_ref[pl.ds(2 * comp, 2)] = up
        down_ref[pl.ds(2 * comp, 2)] = down


def table_of(eps_ref, sig_ref):
    keeps, drives = [], []
    one = jnp.ones((1, 256), F32)
    for index in range(MATS):
        eps = one * eps_ref[index]
        loss = (one * sig_ref[index]) / (2.0 * eps)
        keeps.append((1.0 - loss) / (1.0 + loss))
        drives.append(COURANT / (eps * (1.0 + loss)))
    return keeps, drives


def lookup(code, table):
    keep = jnp.zeros(code.shape, F32)
    drive = jnp.zeros(code.shape, F32)
    for index in range(MATS):
        chosen = code == index + 1.0
        keep = jnp.where(chosen, table[0][index], keep)
        drive = jnp.where(chosen, table[1][index], drive)
    return keep, drive


def wide(own, near_row, strip, corner, slot):
    turn = (128 - 8 * slot) % 128
    if turn:
        strip = pltpu.roll(strip, turn, axis=1)
        corner = pltpu.roll(corner, turn, axis=1)
    return jnp.concatenate(
        (jnp.concatenate((own, strip), axis=1), jnp.concatenate((near_row, corner), axis=1)), axis=0
    )


def ahead(field, axis):
    return pltpu.roll(field, field.shape[axis] - 1, axis=axis)


def behind(field, axis):
    return pltpu.roll(field, 1, axis=axis)


def magnetic(e, e_next, h, rate):
    ex, ey, ez = e
    new_x = h[0] - rate * (ahead(ez, 1) - ez - (e_next[1] - ey))
    new_y = h[1] - rate * (e_next[0] - ex - (ahead(ez, 0) - ez))
    new_z = h[2] - rate * (ahead(ey, 0) - ey - (ahead(ex, 1) - ex))
    return new_x, new_y, new_z


def electric(e, h, h_last, keep, drive):
    hx, hy, hz = h
    new_x = keep * e[0] + drive * (hz - behind(hz, 1) - (hy - h_last[1]))
    new_y = keep * e[1] + drive * (hx - h_last[0] - (hz - behind(hz, 0)))
    new_z = keep * e[2] + drive * (hy - behind(hy, 0) - (hx - behind(hx, 1)))
    return new_x, new_y, new_z


def near_kernel(
    own_ref, down_ref, high_ref, corner_ref, code_ref, eps_ref, sig_ref, near_ref, info_ref
):
    fields = []
    for comp in range(7):
        layers = []
        for z in range(TOP):
            k = comp * TOP + z
            group, slot = divmod(k, 16)
            layers.append(
                wide(own_ref[k], down_ref[k], high_ref[group], corner_ref[group], slot)
            )
        fields.append(layers)
    e = [tuple(fields[c][z] for c in range(3)) for z in range(TOP)]
    h = [tuple(fields[c + 3][z] for c in range(3)) for z in range(TOP)]
    zero = jnp.zeros((16, 256), F32)
    table = table_of(eps_ref, sig_ref)
    coefs = [lookup(fields[6][z], table) for z in range(TOP)]
    last_x, last_y = at_end(GX, True), at_end(GY, True)
    row, lane = sub_iota((16, 256)), lane_iota((16, 256))

    def kept(flag, place, at):
        return 1.0 - (place == at).astype(F32) * flag.astype(F32)

    masks = {
        (0, 1): kept(last_x, row, 7), (1, 1): kept(last_y, lane, 127),
        (0, 0): kept(last_x, row, 8), (1, 0): kept(last_y, lane, 128),
    }

    def over(field, axis):
        return ahead(field, axis) * masks[axis, 1]

    def back(field, axis):
        return behind(field, axis) * masks[axis, 0]

    for step in range(STEPS):
        for z in range(step, TOP):
            ex, ey, ez = e[z]
            e_next = e[z + 1] if z + 1 < TOP else (zero, zero)
            h[z] = (
                h[z][0] - COURANT * (over(ez, 1) - ez - (e_next[1] - ey)),
                h[z][1] - COURANT * (e_next[0] - ex - (over(ez, 0) - ez)),
                h[z][2] - COURANT * (over(ey, 0) - ey - (over(ex, 1) - ex)),
            )
        for z in range(step + 1, TOP):
            keep, drive = coefs[z]
            hx, hy, hz = h[z]
            e[z] = (
                keep * e[z][0] + drive * (hz - back(hz, 1) - (hy - h[z - 1][1])),
                keep * e[z][1] + drive * (hx - h[z - 1][0] - (hz - back(hz, 0))),
                keep * e[z][2] + drive * (hy - back(hy, 0) - (hx - back(hx, 1))),
            )
    tiles = []
    for pol in range(2):
        tile = pltpu.roll(pltpu.roll(e[TOP - 1][pol], 12, axis=0), 252, axis=1)
        tiles.append(tile[:8, :128])
    coded = jnp.dot(
        jnp.concatenate(tiles, axis=0), code_ref[...], precision=lax.Precision.HIGHEST,
        preferred_element_type=F32,
    ).astype(BF16)
    for pol in range(2):
        near_ref[:, pol] = jnp.broadcast_to(coded[8 * pol : 8 * pol + 8], (16, 8, 8, 128))
    lane = lane_iota((8, 128))
    info = own_ref[THIN - 1]
    for k, other in enumerate((high_ref[3], down_ref[THIN - 1], corner_ref[3])):
        info = jnp.where(lane < 8 * k + 8, info, pltpu.roll(other, 8 * k + 8, axis=1))
    info_ref[...] = info


def yee_kernel(
    e_ref, h_ref, mat_ref, up_ref, down_ref, strip_ref, cup_ref, cdown_ref, eps_ref, sig_ref,
    e_out, h_out, e_s, h_s, c_s,
):
    for comp in range(3):
        e_s[comp, NZ] = jnp.zeros((16, 256), F32)
        h_s[comp, 0] = jnp.zeros((16, 256), F32)
    no_up, no_down = at_end(GX, False), at_end(GX, True)
    for comp in range(7):
        near, far = unpair_rows(
            jnp.where(no_up, 0.0, up_ref[pl.ds(32 * comp, 32)]),
            jnp.where(no_down, 0.0, down_ref[pl.ds(32 * comp, 32)]),
        )
        edge = unpair_rows(
            jnp.where(no_up, 0.0, cup_ref[pl.ds(2 * comp, 2)]),
            jnp.where(no_down, 0.0, cdown_ref[pl.ds(2 * comp, 2)]),
        )
        for z in range(NZ):
            group, slot = divmod(z, 16)
            rows = near[z] if z < 32 else far[z - 32]
            own = thin_component(e_ref, h_ref, mat_ref, comp, z)
            value = wide(
                own, rows, strip_ref[4 * comp + group], edge[group // 2][group % 2], slot
            )
            if comp < 3:
                e_s[comp, z] = value
            elif comp < 6:
                h_s[comp - 3, z + 1] = value
            else:
                c_s[2, z] = value

    table = table_of(eps_ref, sig_ref)

    def coef(i, carry):
        for j in range(4):
            z = 4 * i + j
            code = c_s[2, z]
            keep, drive = lookup(code, table)
            c_s[0, z] = keep
            c_s[1, z] = drive
            c_s[2, z] = jnp.where(code > 0.5, COURANT, 0.0)
        return carry

    lax.fori_loop(0, NZ // 4, coef, 0)

    def advance_h(z):
        e = tuple(e_s[c, z] for c in range(3))
        e_next = (e_s[0, z + 1], e_s[1, z + 1])
        h = tuple(h_s[c, z + 1] for c in range(3))
        h = magnetic(e, e_next, h, c_s[2, z])
        for c in range(3):
            h_s[c, z + 1] = h[c]
        return h

    def advance_e(z):
        e = tuple(e_s[c, z] for c in range(3))
        h = tuple(h_s[c, z + 1] for c in range(3))
        return electric(e, h, (h_s[0, z], h_s[1, z]), c_s[0, z], c_s[1, z])

    def step(k, carry):
        def block(i, carry):
            first = i * BLOCK
            for j in range(BLOCK):
                advance_h(first + j)
            for j in range(BLOCK):
                z = first + j
                e = advance_e(z)
                for c in range(3):
                    e_s[c, z] = e[c]
            return carry

        return lax.fori_loop(0, NZ // BLOCK, block, carry)

    lax.fori_loop(0, STEPS - 1, step, 0)

    def final(i, carry):
        first = i * BLOCK
        for j in range(BLOCK):
            z = first + j
            h = advance_h(z)
            for c in range(3):
                h_out[c, z] = h[c][:8, :128]
        for j in range(BLOCK):
            z = first + j
            e = advance_e(z)
            for c in range(3):
                e_out[c, z] = e[c][:8, :128]
        return carry

    lax.fori_loop(0, NZ // BLOCK, final, 0)


def dot(a, b):
    return jnp.dot(a, b, preferred_element_type=F32)


def cut(ref, a, b):
    merged = jnp.where(
        lane_iota((PW, 128)) >= b, ref[0, pl.ds(a, PW), :], ref[1, pl.ds(a, PW), :]
    )
    return pltpu.roll(merged, (128 - b) % 128, axis=1)


def image_kernel(
    place_ref, info_ref, recv_ref, tyh_ref, tyl_ref, txh_ref, txl_ref, second_ref, first_ref,
    up_ref, mask_ref, out_ref, near_s, re_s, im_s, win_s, half_s, acc_s,
):
    for j in range(8):
        tile = recv_ref[:, j].astype(F32).reshape(K, 128)
        near_s[pl.ds(K * (j // 4), K), pl.ds(128 * (j % 4), 128)] = tile.astype(BF16)
    near = near_s[...]
    both = dot(near, tyh_ref[...]) + dot(near, tyl_ref[...])
    half = both[:K] + jnp.where(lane_iota((1, 2 * K)) % 2 == 0, both[K:], -both[K:])
    half_h = half.astype(BF16)
    half_l = (half - half_h.astype(F32)).astype(BF16)
    blocks = dot(txh_ref[...], half_h) + (dot(txh_ref[...], half_l) + dot(txl_ref[...], half_h))
    scale = 1.0 / 512.0
    real = (blocks[:K, :K] + blocks[K:, K:]) * scale
    imag = (blocks[:K, K:] - blocks[K:, :K]) * scale
    real = real.astype(BF16).astype(F32)
    imag = imag.astype(BF16).astype(F32)
    for t in range(2):
        re_s[t] = real[:, 128 * t : 128 * t + 128]
        im_s[t] = imag[:, 128 * t : 128 * t + 128]
    mask = mask_ref[...].astype(F32)
    side = lax.axis_index("x") % 2

    def cuts(i, carry):
        for t in range(8):
            a = place_ref[t, 8 * i]
            b = place_ref[t, 8 * i + 1]
            window = jnp.concatenate(
                (cut(re_s, a, b) * mask, cut(im_s, a, b) * mask), axis=1
            ).astype(BF16)
            win_s[pl.ds(PW * t, PW)] = window
        half = dot(win_s[...], second_ref[side]).astype(BF16)
        for t in range(8):
            rows = half[PW * t : PW * t + PW]
            half_s[i, pl.ds(0, 128), pl.ds(128 * t, 128)] = rows[:, :128]
            half_s[i, pl.ds(128, 128), pl.ds(128 * t, 128)] = rows[:, 128:]
        return carry

    lax.fori_loop(0, 4, cuts, 0)
    acc_s[...] = jnp.zeros(acc_s.shape, F32)

    def fields(i, carry):
        field = dot(first_ref[...], half_s[i])
        power = field[:GRID] * field[:GRID] + field[GRID:] * field[GRID:]
        total = acc_s[...]
        for t in range(8):
            weight = info_ref[t, 8 * i + 2] * (1.0 / SOURCES)
            total = total + power[:, 128 * t : 128 * t + 128] * weight
        acc_s[...] = total
        return carry

    lax.fori_loop(0, 4, fields, 0)
    out_ref[...] = jnp.dot(
        up_ref[...], acc_s[...], precision=lax.Precision.HIGHEST, preferred_element_type=F32
    )


def sum_kernel(recv_ref, up_ref, out_ref):
    total = jnp.sum(recv_ref[...].reshape(64, 8, 128), axis=0)
    total = total + pltpu.roll(total, 4, axis=0)
    line = jnp.concatenate((total, pltpu.roll(total, 6, axis=0)), axis=1)
    full = lax.dot_general(
        line, up_ref[...], (((1,), (1,)), ((), ())), precision=lax.Precision.HIGHEST,
        preferred_element_type=F32,
    )
    out_ref[...] = full[:2]


def shifted(value, axes, by, cyclic=True):
    count = lax.axis_size(axes)
    pairs = [(i, (i + by) % count) for i in range(count)]
    if not cyclic:
        pairs = [(i, j) for i, j in pairs if j == i + by]
    return lax.ppermute(value, axes, pairs)


def diagonal(value):
    rows, cols = lax.axis_size(GX), lax.axis_size(GY)
    pairs = [
        (i * cols + j, (i - 1) % rows * cols + (j - 1) % cols)
        for i in range(rows)
        for j in range(cols)
    ]
    return lax.ppermute(value, ALL, pairs)


def local(
    e_field, h_field, material, permittivity, conductivity, src_shift, src_weight, pupil_mask
):
    rows_all = e_field.shape[2] * lax.axis_size(GX)
    cols_all = e_field.shape[3] * lax.axis_size(GY)
    tyh, tyl, txh, txl, second, first, upsample = map(jnp.asarray, tables(rows_all, cols_all))
    smem = pl.BlockSpec(memory_space=pltpu.SMEM)
    vmem = pl.BlockSpec(memory_space=pltpu.VMEM)

    params = pltpu.CompilerParams(vmem_limit_bytes=28 * 1024 * 1024)

    def here(value):
        return pltpu.with_memory_space_constraint(value, pltpu.VMEM)

    def far(value):
        return pltpu.with_memory_space_constraint(value, pltpu.HBM)

    def shape(*dims, dtype=F32):
        return jax.ShapeDtypeStruct(dims, dtype)

    field = pl.BlockSpec((3, 8, 8, 128), lambda i: (0, 7, 0, 0))
    layer = pl.BlockSpec((8, 8, 128), lambda i: (7, 0, 0))
    thin = pl.BlockSpec((THIN, 8, 128), lambda i: (0, 0, 0))
    head = pl.BlockSpec((4, 8, 128), lambda i: (0, 0, 0))
    thin_x, thin_y = pl.pallas_call(
        thin_kernel,
        grid=(1,),
        out_shape=(shape(THIN, 8, 128), shape(4, 8, 128)),
        in_specs=[field, field, layer, smem, smem],
        out_specs=(thin, head),
        compiler_params=params,
        name="thin",
    )(far(e_field), far(h_field), far(material), far(src_shift.T), far(src_weight))
    next_xy = diagonal(thin_y)
    next_y = shifted(thin_y, GY, -1)
    next_x = shifted(thin_x, GX, -1)
    near, info = pl.pallas_call(
        near_kernel,
        out_shape=(shape(16, 2, 8, 8, 128, dtype=BF16), shape(8, 128)),
        in_specs=[vmem] * 5 + [smem, smem],
        out_specs=(vmem, vmem),
        compiler_params=params,
        name="near",
    )(
        here(thin_x), here(next_x), here(next_y), here(next_xy),
        here(jnp.asarray(cosine_basis().T.astype(np.float32))), permittivity, conductivity,
    )
    recv = lax.all_to_all(near.reshape(256, 8, 128), ALL, 0, 0, tiled=True)

    whole = [vmem, vmem, vmem, pl.BlockSpec(memory_space=pl.ANY)]
    to_low, to_high = pl.pallas_call(
        strip_kernel,
        out_shape=(shape(14, 8, 128), shape(14, 8, 128)),
        in_specs=whole,
        out_specs=(vmem, vmem),
        compiler_params=params,
        name="strip",
    )(e_field, h_field, material, thin_y)
    low = shifted(to_high, GY, 1)
    high = shifted(to_low, GY, -1)
    up, down = pl.pallas_call(
        rows_kernel,
        out_shape=(shape(224, 8, 128), shape(224, 8, 128)),
        in_specs=whole,
        out_specs=(vmem, vmem),
        compiler_params=params,
        name="rows",
    )(e_field, h_field, material, to_low)
    up_in = shifted(up, GX, 1, cyclic=False)
    down_in = shifted(down, GX, -1, cyclic=False)
    strip, cup, cdown = pl.pallas_call(
        corner_kernel,
        out_shape=(shape(28, 8, 128), shape(14, 8, 128), shape(14, 8, 128)),
        in_specs=[vmem] * 2,
        out_specs=(vmem,) * 3,
        compiler_params=params,
        name="corner",
    )(here(low), here(high))
    cup_in = shifted(cup, GX, 1)
    cdown_in = shifted(cdown, GX, -1)

    e_final, h_final = pl.pallas_call(
        yee_kernel,
        out_shape=(shape(*e_field.shape), shape(*h_field.shape)),
        in_specs=[vmem] * 8 + [smem, smem],
        out_specs=(vmem, vmem),
        scratch_shapes=[
            pltpu.VMEM((3, NZ + 1, 16, 256), F32),
            pltpu.VMEM((3, NZ + 1, 16, 256), F32),
            pltpu.VMEM((3, NZ, 16, 256), F32),
        ],
        cost_estimate=pl.CostEstimate(flops=40000000, transcendentals=0, bytes_accessed=8000000),
        compiler_params=params,
        name="yee",
    )(
        e_field, h_field, material, here(up_in), here(down_in), here(strip), here(cup_in),
        here(cdown_in), permittivity, conductivity,
    )

    partial = pl.pallas_call(
        image_kernel,
        out_shape=shape(2 * GRID, 128),
        in_specs=[smem, smem] + [vmem] * 9,
        out_specs=vmem,
        scratch_shapes=[
            pltpu.VMEM((2 * K, 512), BF16),
            pltpu.VMEM((2, K, 128), F32),
            pltpu.VMEM((2, K, 128), F32),
            pltpu.VMEM((8 * PW, 256), BF16),
            pltpu.VMEM((4, 256, 1024), BF16),
            pltpu.VMEM((GRID, 128), F32),
        ],
        compiler_params=params,
        name="image",
    )(
        info.astype(jnp.int32), info, here(recv.reshape(32, 8, 8, 128)), far(tyh), far(tyl),
        far(txh), far(txl), far(second), far(first), far(upsample), far(pupil_mask),
    )
    pieces = lax.all_to_all(partial.reshape(256, 2, 128), ALL, 0, 0, tiled=True)
    image = pl.pallas_call(
        sum_kernel,
        out_shape=shape(2, IMG),
        in_specs=[vmem, vmem],
        out_specs=vmem,
        compiler_params=params,
        name="total",
    )(here(pieces.reshape(512, 128)), here(upsample))
    return image, e_final, h_final


def solution(mesh):
    finer = Mesh(mesh.devices.reshape(4, 4, 2, 2, 4), ALL)
    return jax.shard_map(
        local,
        mesh=finer,
        in_specs=(
            P(None, None, GX, GY),
            P(None, None, GX, GY),
            P(None, GX, GY),
            P(),
            P(),
            P(ALL, None),
            P(ALL),
            P(),
        ),
        out_specs=(P(ALL, None), P(None, None, GX, GY), P(None, None, GX, GY)),
        check_vma=False,
    )
```
